128 devices in a mesh: dp: 8 (over z, core), expert: 16 (over y, x).
Axes of the slice: x: 4, y: 4, z: 4, core: 2. Of those that a mesh axis runs over, the one named last changes fastest.
Arguments:
- tokens: bfloat16 [131072, 2080], P(('dp', 'expert')), may hold values from -6 to 6
- router_logits: bfloat16 [131072, 2048], P(('dp', 'expert')), may hold values from -300 to 300
- gate_grad: float32 [131072], P(('dp', 'expert')), may hold values from -6 to 6
- expert_index: int32 [131072, 1], P(('dp', 'expert')), may hold values from 0 to 2047
- keep_mask: int32 [2048], replicated, may hold values 0 or 1
Outputs:
- router_grad: float32 [2048, 2080], P('expert', 'dp')
The draws below stay inside these ranges and needn't reach their ends.
All inputs are finite; a program needn't handle non-finite values.
Results may differ from the reference program's by a relative error of at most 0.0003.
Values sent between devices are 32-bit elements; how exact they have to be, the bound alone decides.
A program may use at most 128 MiB of HBM per device.

```python
import math
import jax
import jax.numpy as jnp
from jax import lax

D = 2080
E = 2048
TOKENS = 131072


def draw_router_logits(key, part):
    first_key, second_key, third_key = jax.random.split(jax.random.fold_in(key, 17), 3)
    values = 2.0 * jax.random.normal(first_key, (TOKENS, E), jnp.float32)
    return values.astype(jnp.bfloat16)


def touch_ends(array, stream_key, least, high):
    longest = array.shape.index(max(array.shape))
    spots = []
    for shift in (0, 1):
        where = [jax.random.randint(jax.random.fold_in(stream_key, axis), (), 0, length) for axis, length in enumerate(array.shape)]
        where[longest] = (where[longest] + shift) % array.shape[longest]
        spots.append(tuple(where))
    return array.at[spots[0]].set(least).at[spots[1]].set(high)


def level_of(key, extent, shards, smallest, top_value):
    def one(position, shards_of):
        heights = jax.random.uniform(jax.random.fold_in(jax.random.fold_in(key, 6), position), (shards_of,), jnp.float32, smallest / len(shards), top_value / len(shards))
        return jnp.repeat(jnp.exp(heights), extent[position] // shards_of).reshape((-1,) + (1,) * (len(extent) - position - 1))

    gain = one(*shards[0])
    for cut in shards[1:]:
        gain = gain * one(*cut)
    return gain


def different_ones(rng, rows, amount, top, lift):
    order = jax.random.permutation(jax.random.fold_in(rng, 1), amount)
    boost = order
    for power in range(3):
        boost = boost * boost // amount
    boost = boost * lift // amount
    lots = jax.random.randint(jax.random.fold_in(rng, 2), (rows, amount), 0, 4096) + boost
    fixed_rows = jax.random.permutation(jax.random.fold_in(rng, 3), rows)[jnp.arange(amount) % rows]
    lots = jnp.where(jnp.arange(rows)[:, None] == fixed_rows[None, :], 1 << 14, lots)
    priority = lots * amount + jnp.arange(amount)
    return lax.top_k(priority.astype(jnp.int32), top)[1].astype(jnp.int32)


def bell_draw(stream_key, extent, width, bound, cuts=(), kind=jnp.bfloat16):
    result = jax.random.normal(stream_key, extent, jnp.float32) * width
    if len(cuts) > 0:
        result = level_of(stream_key, extent, cuts, -0.22, 0.18) * result
    return jnp.clip(result, min=-bound, max=bound).astype(kind)


def setup_inputs(seed: int = 0) -> dict:
    arg_keys = jax.random.split(jax.random.key(seed), 6)
    tokens = bell_draw(arg_keys[0], (TOKENS, D), 1.0, 6.0, ((0, 128),))
    router_logits = draw_router_logits(jax.random.fold_in(arg_keys[5], 71), 0)
    gate_grad = bell_draw(arg_keys[2], (TOKENS,), 1.0, 6.0, ((0, 128),), jnp.float32)
    expert_index = different_ones(arg_keys[3], TOKENS, E, 1, 8)
    keep_mask = touch_ends((jax.random.randint(arg_keys[4], (E,), 0, 8) < 7).astype(jnp.int32), jax.random.fold_in(arg_keys[4], 1), 0, 1)
    return dict(tokens=tokens, router_logits=router_logits, gate_grad=gate_grad, expert_index=expert_index, keep_mask=keep_mask)


def logit_gradient(logit_block, gate_block, routed_block, aux_cost, kept_cols):
    scores = logit_block.astype(jnp.float32)
    row_peak = jnp.max(scores, axis=1, keepdims=True)
    weights = jnp.exp(scores - row_peak)
    router_probs = weights / jnp.sum(weights, axis=1, keepdims=True)
    columns = lax.broadcasted_iota(jnp.int32, scores.shape, 1)
    chosen = columns == routed_block[:, None]
    top_prob = jnp.sum(jnp.where(chosen, router_probs, 0.0), axis=1)
    spread = jnp.dot(router_probs, aux_cost, precision=lax.Precision.HIGHEST)
    gate_part = (gate_block * top_prob)[:, None] * (chosen.astype(jnp.float32) - router_probs)
    aux_part = router_probs * (aux_cost[None, :] - spread[:, None])
    return kept_cols[None, :] * (gate_part + aux_part)


def reference(tokens, router_logits, gate_grad, expert_index, keep_mask):
    routed = expert_index[:, 0].astype(jnp.int32)
    total_tokens = tokens.shape[0]
    expert_total = router_logits.shape[1]
    counts = jax.ops.segment_sum(jnp.ones((total_tokens,), jnp.int32), routed, num_segments=expert_total)
    aux_cost = counts.astype(jnp.float32) * (expert_total / total_tokens)
    kept_cols = keep_mask.astype(jnp.float32)
    block_rows = math.gcd(total_tokens, 4096)
    offsets = jnp.arange(total_tokens // block_rows, dtype=jnp.int32) * block_rows

    def advance(running, offset):
        token_block = lax.dynamic_slice_in_dim(tokens, offset, block_rows, 0)
        logit_block = lax.dynamic_slice_in_dim(router_logits, offset, block_rows, 0)
        gate_block = lax.dynamic_slice_in_dim(gate_grad, offset, block_rows, 0)
        routed_block = lax.dynamic_slice_in_dim(routed, offset, block_rows, 0)
        grad_block = logit_gradient(logit_block, gate_block, routed_block, aux_cost, kept_cols)
        running = running + lax.dot_general(grad_block.astype(jnp.float32), token_block.astype(jnp.float32), (((0,), (0,)), ((), ())), precision=lax.Precision.HIGHEST, preferred_element_type=jnp.float32)
        return running, None

    start_value = jnp.zeros((expert_total, tokens.shape[1]), jnp.float32)
    final, unused = lax.scan(advance, start_value, offsets)
    return final
```

```python
import functools

import jax
import jax.numpy as jnp
from jax import lax
from jax.experimental import pallas as pl
from jax.experimental.pallas import tpu as pltpu
from jax.sharding import PartitionSpec as P

MESH = pl.DeviceIdType.MESH
RING = 4
LANES = 128
ROW_CHUNKS = (8, 16, 16, 16, 16, 16)
TB = 128


def kernel(total_tokens, idx_ref, gate_ref, keep_ref, tok_ref, logit_ref, out_ref,
           lbuf, xbuf, icol, acol, invc, ptab, gmat, xf, xt, cbuf, drecv, sums, r1m, r1f, tmid, r2, umid, r3,
           fin, cnt, cnt_recv, aux_ref,
           lsem, xsem, csend, crecv, dsend, drsem, ssem, rsem):
    tok_rows, d_model = tok_ref.shape
    experts = logit_ref.shape[1]
    eblocks = experts // LANES
    blocks = tok_rows // TB
    chunks = len(ROW_CHUNKS)
    offsets = [sum(ROW_CHUNKS[:k]) for k in range(chunks)]

    dp = lax.axis_index("dp")
    ex = lax.axis_index("expert")
    zc, core = dp // 2, dp % 2
    yc, xc = ex // RING, ex % RING
    here = {"x": xc, "y": yc, "z": zc}

    def device(**moved):
        at = dict(here, **moved)
        return (2 * at["z"] + core, RING * at["y"] + at["x"])

    sibling = (2 * zc + 1 - core, ex)

    def away(axis, step):
        return device(**{axis: (here[axis] + step) % RING})

    def load_logits(b, slot):
        return pltpu.make_async_copy(logit_ref.at[pl.ds(b * TB, TB), :], lbuf.at[slot], lsem.at[slot])

    def load_tokens(b, slot):
        return pltpu.make_async_copy(tok_ref.at[pl.ds(b * TB, TB), :], xbuf.at[slot], xsem.at[slot])

    load_logits(0, 0).start()
    load_logits(1, 1).start()
    load_tokens(0, 0).start()
    load_tokens(1, 1).start()

    barrier = pltpu.get_barrier_semaphore()
    peers = [sibling] + [away(axis, step) for axis in "xyz" for step in (1, 2, 3)]
    for peer in peers:
        pl.semaphore_signal(barrier, inc=1, device_id=peer, device_id_type=MESH)

    idx = idx_ref[...]
    total = jnp.zeros((eblocks, LANES), jnp.float32)
    for b in range(blocks):
        row = idx[b : b + 1, :]
        high = (row // LANES == lax.broadcasted_iota(jnp.int32, (eblocks, LANES), 0)).astype(jnp.bfloat16)
        low = (row % LANES == lax.broadcasted_iota(jnp.int32, (LANES, LANES), 0)).astype(jnp.bfloat16)
        total = total + lax.dot_general(high, low, (((1,), (1,)), ((), ())), preferred_element_type=jnp.float32)
    cnt[0] = total.astype(jnp.int32)

    pl.semaphore_wait(barrier, len(peers))

    def count_copies(stage):
        if stage == 0:
            return [pltpu.make_async_remote_copy(cnt.at[0], cnt_recv.at[0], csend.at[0], crecv.at[0], device_id=sibling, device_id_type=MESH)]
        axis = "xyz"[stage - 1]
        copies = []
        for step in (1, 2, 3):
            slot = 1 + 3 * (stage - 1) + step - 1
            copies.append(pltpu.make_async_remote_copy(
                cnt.at[stage], cnt_recv.at[slot], csend.at[slot], crecv.at[slot], device_id=away(axis, step), device_id_type=MESH))
        return copies

    def count_arrive(stage):
        value = cnt[stage]
        for number, copy in enumerate(count_copies(stage)):
            copy.wait_recv()
            slot = 0 if stage == 0 else 1 + 3 * (stage - 1) + number
            value = value + cnt_recv[slot]
        return value

    def count_step(stage):
        cnt[stage + 1] = count_arrive(stage)
        for copy in count_copies(stage + 1):
            copy.start()

    for copy in count_copies(0):
        copy.start()

    idx_t = jnp.transpose(idx.astype(jnp.float32))
    gate_t = jnp.transpose(gate_ref[...])
    for b in range(blocks):
        icol[b * TB : (b + 1) * TB, :] = jnp.broadcast_to(idx_t[:, b : b + 1], (TB, LANES)).astype(jnp.int32)
        acol[b * TB : (b + 1) * TB, :] = jnp.broadcast_to(gate_t[:, b : b + 1], (TB, LANES))

    RS = 32

    def lane_of(j):
        return lax.broadcasted_iota(jnp.int32, (RS, LANES), 1) + j * LANES

    def stats_block(b):
        slot = b % 2
        load_logits(b, slot).wait()

        def rows(r, carry):
            local = pl.ds(pl.multiple_of(r * RS, RS), RS)
            at = pl.ds(pl.multiple_of(b * TB + r * RS, RS), RS)
            peak = lbuf[slot, local, 0:LANES].astype(jnp.float32)
            for j in range(1, eblocks):
                peak = jnp.maximum(peak, lbuf[slot, local, j * LANES : (j + 1) * LANES].astype(jnp.float32))
            peak = jnp.max(peak, axis=1, keepdims=True)
            mass = jnp.zeros((RS, LANES), jnp.float32)
            top = jnp.zeros((RS, LANES), jnp.float32)
            chosen = icol[at, :]
            for j in range(eblocks):
                weight = jnp.exp(lbuf[slot, local, j * LANES : (j + 1) * LANES].astype(jnp.float32) - peak)
                ptab[at, j * LANES : (j + 1) * LANES] = weight
                mass = mass + weight
                top = top + jnp.where(chosen == lane_of(j), weight, 0.0)
            inverse = 1.0 / jnp.sum(mass, axis=1, keepdims=True)
            top_prob = jnp.sum(top, axis=1, keepdims=True) * inverse
            invc[at, :] = jnp.broadcast_to(inverse, (RS, LANES))
            acol[at, :] = acol[at, :] * top_prob
            return carry

        lax.fori_loop(0, TB // RS, rows, 0)

    def xpose_block(b):
        slot = b % 2
        load_tokens(b, slot).wait()
        for c in range(0, d_model, LANES):
            width = min(LANES, d_model - c)
            xf[c : c + width, :] = jnp.transpose(xbuf[slot, :, c : c + width].astype(jnp.float32))
        cols = pl.ds(pl.multiple_of(b * TB, TB), TB)
        for k in range(chunks):
            r = ROW_CHUNKS[k]
            pieces = []
            for group in range(24):
                cc, zz, part = group // 12, (group // 3) % 4, group % 3
                src = (d_model // RING) * zz + 256 * cc + 88 * part + offsets[k]
                pieces.append(xf[src : src + r, :])
            dst = 24 * offsets[k]
            if r == 8:
                for g in range(0, 24, 2):
                    xt[dst + 8 * g : dst + 8 * g + 16, cols] = jnp.concatenate([pieces[g], pieces[g + 1]], axis=0).astype(jnp.bfloat16)
            else:
                for g in range(24):
                    xt[dst + r * g : dst + r * (g + 1), cols] = pieces[g].astype(jnp.bfloat16)

    def prep(b, carry):
        stats_block(b)

        @pl.when(b + 2 < blocks)
        def _():
            load_logits(b + 2, b % 2).start()

        xpose_block(b)

        @pl.when(b + 2 < blocks)
        def _():
            load_tokens(b + 2, b % 2).start()

        return carry

    lax.fori_loop(0, 2, prep, 0)
    count_step(0)
    lax.fori_loop(2, 4, prep, 0)
    count_step(1)
    lax.fori_loop(4, 7, prep, 0)
    count_step(2)
    lax.fori_loop(7, 8, prep, 0)

    aux_ref[...] = count_arrive(3).astype(jnp.float32) * (experts / total_tokens)
    aux = aux_ref[...]

    def grad_rows(r, carry):
        at = pl.ds(pl.multiple_of(r * RS, RS), RS)
        acc = ptab[at, 0:LANES] * aux[0:1, :]
        for j in range(1, eblocks):
            acc = acc + ptab[at, j * LANES : (j + 1) * LANES] * aux[j : j + 1, :]
        inverse = invc[at, :]
        spread = jnp.sum(acc, axis=1, keepdims=True) * inverse
        gain = acol[at, :]
        drop = spread + gain
        chosen = icol[at, :]
        for j in range(eblocks):
            value = (ptab[at, j * LANES : (j + 1) * LANES] * inverse) * (aux[j : j + 1, :] - drop)
            value = value + jnp.where(chosen == lane_of(j), gain, 0.0)
            big = value.astype(jnp.bfloat16)
            gmat[0, at, j * LANES : (j + 1) * LANES] = big
            gmat[1, at, j * LANES : (j + 1) * LANES] = (value - big.astype(jnp.float32)).astype(jnp.bfloat16)
        return carry

    lax.fori_loop(0, tok_rows // RS, grad_rows, 0)

    NT = 256

    def pair_copy(k):
        rows = 12 * ROW_CHUNKS[k]
        src = cbuf.at[k % 2, :, pl.ds(pl.multiple_of((1 - core) * rows, 8), rows), :]
        return pltpu.make_async_remote_copy(src, drecv[k], dsend.at[k], drsem.at[k], device_id=sibling, device_id_type=MESH)

    def matmul_chunk(k):
        if k >= 2:
            pair_copy(k - 2).wait_send()
        rows = 24 * ROW_CHUNKS[k]
        base = 24 * offsets[k]

        def tile(n, carry):
            cols = pl.ds(pl.multiple_of(n * NT, NT), NT)
            left = xt[base : base + rows, :]
            value = jnp.dot(left, gmat[0, :, cols], preferred_element_type=jnp.float32)
            value = value + jnp.dot(left, gmat[1, :, cols], preferred_element_type=jnp.float32)
            for half in range(NT // LANES):
                cbuf[k % 2, n * (NT // LANES) + half, 0:rows, :] = value[:, half * LANES : (half + 1) * LANES]
            return carry

        lax.fori_loop(0, experts // NT, tile, 0)
        pair_copy(k).start()

    orders = ("xyz", "yzx", "zxy")

    def rcopy(k, p, n, src, dst, peer):
        return pltpu.make_async_remote_copy(src, dst, ssem.at[k, p, n], rsem.at[k, p, n], device_id=peer, device_id_type=MESH)

    def pos(p, stage):
        return here[orders[p][stage]]

    def ring1(k, p, numbers):
        axis = orders[p][0]
        i = pos(p, 0)
        up, down, far = (i + 1) % RING, (i + 3) % RING, (i + 2) % RING
        right, left = away(axis, 1), away(axis, 3)
        s, m, f = sums[k], r1m[k], r1f[k]
        table = (
            (s.at[p, far, 0:2], m.at[p, 0], right),
            (s.at[p, far, 2:4], m.at[p, 1], left),
            (s.at[p, up, 2:4], f.at[p, 0, 2:4], right),
            (s.at[p, down, 0:2], f.at[p, 1, 0:2], left),
            (s.at[p, up, 0:2], f.at[p, 0, 0:2], right),
            (s.at[p, down, 2:4], f.at[p, 1, 2:4], left),
        )
        return [rcopy(k, p, n, *table[n]) for n in numbers]

    def ring2(k, p):
        axis, i = orders[p][1], pos(p, 1)
        return [rcopy(k, p, 5 + step, tmid[k].at[p, (i + step) % RING], r2[k].at[p, step - 1], away(axis, step)) for step in (1, 2, 3)]

    def ring3(k, p):
        axis, i = orders[p][2], pos(p, 2)
        return [rcopy(k, p, 8 + step, umid[k].at[p, (i + step) % RING], r3[k].at[p, step - 1], away(axis, step)) for step in (1, 2, 3)]

    def stage_a(k):
        pair_copy(k).wait_recv()
        r = ROW_CHUNKS[k]

        def block(e, carry):
            ye, xe = e // RING, e % RING
            for zz in range(RING):
                for p in range(3):
                    row = (zz * 3 + p) * r
                    mine = pl.ds(pl.multiple_of(core * (12 * r) + row, 8), r)
                    value = cbuf[k % 2, e, mine, :] + drecv[k][e, row : row + r, :]
                    at = {"x": xe, "y": ye, "z": zz}
                    sums[k][p, at[orders[p][0]], at[orders[p][1]], at[orders[p][2]]] = value
            return carry

        lax.fori_loop(0, eblocks, block, 0)
        for n in range(4):
            for p in range(3):
                ring1(k, p, (n,))[0].start()

    def stage_b(k):
        for p in range(3):
            i = pos(p, 0)
            up, down = (i + 1) % RING, (i + 3) % RING
            copies = ring1(k, p, (0, 1, 4, 5))
            copies[0].wait_recv()
            sums[k][p, up, 0:2] = sums[k][p, up, 0:2] + r1m[k][p, 0]
            copies[2].start()
            copies[1].wait_recv()
            sums[k][p, down, 2:4] = sums[k][p, down, 2:4] + r1m[k][p, 1]
            copies[3].start()

    def stage_c(k):
        for p in range(3):
            i = pos(p, 0)
            for copy in ring1(k, p, (2, 3, 4, 5)):
                copy.wait_recv()
            tmid[k][p] = sums[k][p, i] + r1f[k][p, 0] + r1f[k][p, 1]
            for copy in ring2(k, p):
                copy.start()

    def stage_d(k):
        for p in range(3):
            for copy in ring2(k, p):
                copy.wait_recv()
            umid[k][p] = tmid[k][p, pos(p, 1)] + r2[k][p, 0] + r2[k][p, 1] + r2[k][p, 2]
            for copy in ring3(k, p):
                copy.start()

    def stage_e(k):
        r = ROW_CHUNKS[k]
        for p in range(3):
            for copy in ring3(k, p):
                copy.wait_recv()
            row = 88 * p + offsets[k]
            fin[row : row + r, :] = umid[k][p, pos(p, 2)] + r3[k][p, 0] + r3[k][p, 1] + r3[k][p, 2]

    stages = (matmul_chunk, stage_a, stage_b, stage_c, stage_d, stage_e)
    for turn in range(chunks + len(stages) - 1):
        for lag, stage in enumerate(stages):
            if 0 <= turn - lag < chunks:
                stage(turn - lag)

    keep = keep_ref[pl.ds(ex, 1), :].astype(jnp.float32)
    rows = d_model // 8
    whole = fin[...] * keep
    first, second = whole[0:rows, :], whole[whole.shape[0] - rows :, :]
    out_ref[...] = jnp.transpose(jnp.where(core == 0, first, second))

    for stage in range(4):
        for copy in count_copies(stage):
            copy.wait_send()
    for k in range(max(chunks - 2, 0), chunks):
        pair_copy(k).wait_send()
    for k in range(chunks):
        for p in range(3):
            for copy in ring1(k, p, range(6)) + ring2(k, p) + ring3(k, p):
                copy.wait_send()


def solution(mesh):
    devices = mesh.devices.size

    def local(tokens, router_logits, gate_grad, expert_index, keep_mask):
        tok_rows, d_model = tokens.shape
        experts = router_logits.shape[1]
        eblocks = experts // LANES
        chunks = len(ROW_CHUNKS)
        f32, bf16, i32 = jnp.float32, jnp.bfloat16, jnp.int32
        rmax = max(ROW_CHUNKS)
        vm = pltpu.VMEM

        def per_chunk(shape_of):
            return [vm(shape_of(r), f32) for r in ROW_CHUNKS]

        scratch = [
            vm((2, TB, experts), bf16),
            vm((2, TB, d_model), bf16),
            vm((tok_rows, LANES), i32),
            vm((tok_rows, LANES), f32),
            vm((tok_rows, LANES), f32),
            vm((tok_rows, experts), f32),
            vm((2, tok_rows, experts), bf16),
            vm((d_model, TB), f32),
            vm((24 * sum(ROW_CHUNKS), tok_rows), bf16),
            vm((2, eblocks, 24 * rmax, LANES), f32),
            per_chunk(lambda r: (eblocks, 12 * r, LANES)),
            per_chunk(lambda r: (3, 4, 4, 4, r, LANES)),
            per_chunk(lambda r: (3, 2, 2, 4, r, LANES)),
            per_chunk(lambda r: (3, 2, 4, 4, r, LANES)),
            per_chunk(lambda r: (3, 4, 4, r, LANES)),
            per_chunk(lambda r: (3, 3, 4, r, LANES)),
            per_chunk(lambda r: (3, 4, r, LANES)),
            per_chunk(lambda r: (3, 3, r, LANES)),
            vm((264, LANES), f32),
            vm((4, eblocks, LANES), i32),
            vm((10, eblocks, LANES), i32),
            vm((eblocks, LANES), f32),
            pltpu.SemaphoreType.DMA((2,)),
            pltpu.SemaphoreType.DMA((2,)),
            pltpu.SemaphoreType.DMA((10,)),
            pltpu.SemaphoreType.DMA((10,)),
            pltpu.SemaphoreType.DMA((chunks,)),
            pltpu.SemaphoreType.DMA((chunks,)),
            pltpu.SemaphoreType.DMA((chunks, 3, 12)),
            pltpu.SemaphoreType.DMA((chunks, 3, 12)),
        ]
        return pl.pallas_call(
            functools.partial(kernel, tok_rows * devices),
            out_shape=jax.ShapeDtypeStruct((LANES, d_model // 8), f32),
            in_specs=[pl.BlockSpec(memory_space=pltpu.VMEM)] * 3 + [pl.BlockSpec(memory_space=pl.ANY)] * 2,
            out_specs=pl.BlockSpec(memory_space=pltpu.VMEM),
            scratch_shapes=scratch,
            compiler_params=pltpu.CompilerParams(collective_id=0, has_side_effects=True, vmem_limit_bytes=67043328),
        )(
            expert_index.reshape(tok_rows // LANES, LANES),
            gate_grad.reshape(tok_rows // LANES, LANES),
            keep_mask.reshape(eblocks, LANES),
            tokens,
            router_logits,
        )

    return jax.shard_map(
        local,
        mesh=mesh,
        in_specs=(P(("dp", "expert"), None), P(("dp", "expert"), None), P(("dp", "expert")), P(("dp", "expert"), None), P()),
        out_specs=P("expert", "dp"),
        check_vma=False,
    )
```

```python
import functools

import jax
import jax.numpy as jnp
from jax import lax
from jax.experimental import pallas as pl
from jax.experimental.pallas import tpu as pltpu
from jax.sharding import PartitionSpec as P

MESH = pl.DeviceIdType.MESH
RING = 4
LANES = 128
ROW_CHUNKS = (8, 16, 16, 16, 16, 16)
TB = 128


def kernel(total_tokens, idx_ref, gate_ref, keep_ref, tok_ref, logit_ref, out_ref,
           lbuf, icol, acol, invc, ptab, gmat, xt, cbuf, drecv, sums, r1m, r1f, tmid, r2, umid, r3,
           fin, cnt, cnt_recv, aux_ref,
           lsem, xsem, csend, crecv, dsend, drsem, ssem, rsem):
    d_model, tok_rows = tok_ref.shape
    experts = logit_ref.shape[1]
    eblocks = experts // LANES
    blocks = tok_rows // TB
    chunks = len(ROW_CHUNKS)
    offsets = [sum(ROW_CHUNKS[:k]) for k in range(chunks)]

    dp = lax.axis_index("dp")
    ex = lax.axis_index("expert")
    zc, core = dp // 2, dp % 2
    yc, xc = ex // RING, ex % RING
    here = {"x": xc, "y": yc, "z": zc}

    def device(**moved):
        at = dict(here, **moved)
        return (2 * at["z"] + core, RING * at["y"] + at["x"])

    sibling = (2 * zc + 1 - core, ex)

    def away(axis, step):
        return device(**{axis: (here[axis] + step) % RING})

    def load_logits(b, slot):
        return pltpu.make_async_copy(logit_ref.at[pl.ds(b * TB, TB), :], lbuf.at[slot], lsem.at[slot])

    for k in range(chunks):
        r = ROW_CHUNKS[k]
        for group in range(24):
            cc, zz, part = group // 12, (group // 3) % 4, group % 3
            src = (d_model // RING) * zz + 256 * cc + 88 * part + offsets[k]
            dst = 24 * offsets[k] + r * group
            pltpu.make_async_copy(tok_ref.at[pl.ds(src, r), :], xt.at[pl.ds(dst, r), :], xsem.at[k]).start()

    load_logits(0, 0).start()
    load_logits(1, 1).start()

    barrier = pltpu.get_barrier_semaphore()
    peers = [sibling] + [away(axis, step) for axis in "xyz" for step in (1, 2, 3)]
    for peer in peers:
        pl.semaphore_signal(barrier, inc=1, device_id=peer, device_id_type=MESH)

    idx = idx_ref[...]
    total = jnp.zeros((eblocks, LANES), jnp.float32)
    for b in range(blocks):
        row = idx[b : b + 1, :]
        high = (row // LANES == lax.broadcasted_iota(jnp.int32, (eblocks, LANES), 0)).astype(jnp.bfloat16)
        low = (row % LANES == lax.broadcasted_iota(jnp.int32, (LANES, LANES), 0)).astype(jnp.bfloat16)
        total = total + lax.dot_general(high, low, (((1,), (1,)), ((), ())), preferred_element_type=jnp.float32)
    cnt[0] = total.astype(jnp.int32)

    pl.semaphore_wait(barrier, len(peers))

    def count_copies(stage):
        if stage == 0:
            return [pltpu.make_async_remote_copy(cnt.at[0], cnt_recv.at[0], csend.at[0], crecv.at[0], device_id=sibling, device_id_type=MESH)]
        axis = "xyz"[stage - 1]
        copies = []
        for step in (1, 2, 3):
            slot = 1 + 3 * (stage - 1) + step - 1
            copies.append(pltpu.make_async_remote_copy(
                cnt.at[stage], cnt_recv.at[slot], csend.at[slot], crecv.at[slot], device_id=away(axis, step), device_id_type=MESH))
        return copies

    def count_arrive(stage):
        value = cnt[stage]
        for number, copy in enumerate(count_copies(stage)):
            copy.wait_recv()
            slot = 0 if stage == 0 else 1 + 3 * (stage - 1) + number
            value = value + cnt_recv[slot]
        return value

    def count_step(stage):
        cnt[stage + 1] = count_arrive(stage)
        for copy in count_copies(stage + 1):
            copy.start()

    for copy in count_copies(0):
        copy.start()

    idx_t = jnp.transpose(idx.astype(jnp.float32))
    gate_t = jnp.transpose(gate_ref[...])
    for b in range(blocks):
        icol[b * TB : (b + 1) * TB, :] = jnp.broadcast_to(idx_t[:, b : b + 1], (TB, LANES)).astype(jnp.int32)
        acol[b * TB : (b + 1) * TB, :] = jnp.broadcast_to(gate_t[:, b : b + 1], (TB, LANES))

    RS = 32

    def lane_of(j):
        return lax.broadcasted_iota(jnp.int32, (RS, LANES), 1) + j * LANES

    def stats_block(b):
        slot = b % 2
        load_logits(b, slot).wait()

        def rows(r, carry):
            local = pl.ds(pl.multiple_of(r * RS, RS), RS)
            at = pl.ds(pl.multiple_of(b * TB + r * RS, RS), RS)
            peak = lbuf[slot, local, 0:LANES].astype(jnp.float32)
            for j in range(1, eblocks):
                peak = jnp.maximum(peak, lbuf[slot, local, j * LANES : (j + 1) * LANES].astype(jnp.float32))
            peak = jnp.max(peak, axis=1, keepdims=True)
            mass = jnp.zeros((RS, LANES), jnp.float32)
            top = jnp.zeros((RS, LANES), jnp.float32)
            chosen = icol[at, :]
            for j in range(eblocks):
                weight = jnp.exp(lbuf[slot, local, j * LANES : (j + 1) * LANES].astype(jnp.float32) - peak)
                ptab[at, j * LANES : (j + 1) * LANES] = weight
                mass = mass + weight
                top = top + jnp.where(chosen == lane_of(j), weight, 0.0)
            inverse = 1.0 / jnp.sum(mass, axis=1, keepdims=True)
            top_prob = jnp.sum(top, axis=1, keepdims=True) * inverse
            invc[at, :] = jnp.broadcast_to(inverse, (RS, LANES))
            acol[at, :] = acol[at, :] * top_prob
            return carry

        lax.fori_loop(0, TB // RS, rows, 0)

    def prep(b, carry):
        stats_block(b)

        @pl.when(b + 2 < blocks)
        def _():
            load_logits(b + 2, b % 2).start()

        return carry

    lax.fori_loop(0, 2, prep, 0)
    count_step(0)
    lax.fori_loop(2, 4, prep, 0)
    count_step(1)
    lax.fori_loop(4, 7, prep, 0)
    count_step(2)
    lax.fori_loop(7, 8, prep, 0)

    aux_ref[...] = count_arrive(3).astype(jnp.float32) * (experts / total_tokens)
    aux = aux_ref[...]

    def grad_rows(r, carry):
        at = pl.ds(pl.multiple_of(r * RS, RS), RS)
        acc = ptab[at, 0:LANES] * aux[0:1, :]
        for j in range(1, eblocks):
            acc = acc + ptab[at, j * LANES : (j + 1) * LANES] * aux[j : j + 1, :]
        inverse = invc[at, :]
        spread = jnp.sum(acc, axis=1, keepdims=True) * inverse
        gain = acol[at, :]
        drop = spread + gain
        chosen = icol[at, :]
        for j in range(eblocks):
            value = (ptab[at, j * LANES : (j + 1) * LANES] * inverse) * (aux[j : j + 1, :] - drop)
            value = value + jnp.where(chosen == lane_of(j), gain, 0.0)
            big = value.astype(jnp.bfloat16)
            gmat[0, at, j * LANES : (j + 1) * LANES] = big
            gmat[1, at, j * LANES : (j + 1) * LANES] = (value - big.astype(jnp.float32)).astype(jnp.bfloat16)
        return carry

    lax.fori_loop(0, tok_rows // RS, grad_rows, 0)

    NT = 256

    def pair_copy(k):
        rows = 12 * ROW_CHUNKS[k]
        src = cbuf.at[k % 2, :, pl.ds(pl.multiple_of((1 - core) * rows, 8), rows), :]
        return pltpu.make_async_remote_copy(src, drecv[k], dsend.at[k], drsem.at[k], device_id=sibling, device_id_type=MESH)

    def matmul_chunk(k):
        if k >= 2:
            pair_copy(k - 2).wait_send()
        rows = 24 * ROW_CHUNKS[k]
        base = 24 * offsets[k]
        chunk_rows = xt.at[pl.ds(base, rows), :]
        pltpu.make_async_copy(chunk_rows, chunk_rows, xsem.at[k]).wait()

        def tile(n, carry):
            cols = pl.ds(pl.multiple_of(n * NT, NT), NT)
            left = xt[base : base + rows, :]
            value = jnp.dot(left, gmat[0, :, cols], preferred_element_type=jnp.float32)
            value = value + jnp.dot(left, gmat[1, :, cols], preferred_element_type=jnp.float32)
            for half in range(NT // LANES):
                cbuf[k % 2, n * (NT // LANES) + half, 0:rows, :] = value[:, half * LANES : (half + 1) * LANES]
            return carry

        lax.fori_loop(0, experts // NT, tile, 0)
        pair_copy(k).start()

    orders = ("xyz", "yzx", "zxy")

    def rcopy(k, p, n, src, dst, peer):
        return pltpu.make_async_remote_copy(src, dst, ssem.at[k, p, n], rsem.at[k, p, n], device_id=peer, device_id_type=MESH)

    def pos(p, stage):
        return here[orders[p][stage]]

    def ring1(k, p, numbers):
        axis = orders[p][0]
        i = pos(p, 0)
        up, down, far = (i + 1) % RING, (i + 3) % RING, (i + 2) % RING
        right, left = away(axis, 1), away(axis, 3)
        s, m, f = sums[k], r1m[k], r1f[k]
        table = (
            (s.at[p, far, 0:2], m.at[p, 0], right),
            (s.at[p, far, 2:4], m.at[p, 1], left),
            (s.at[p, up, 2:4], f.at[p, 0, 2:4], right),
            (s.at[p, down, 0:2], f.at[p, 1, 0:2], left),
            (s.at[p, up, 0:2], f.at[p, 0, 0:2], right),
            (s.at[p, down, 2:4], f.at[p, 1, 2:4], left),
        )
        return [rcopy(k, p, n, *table[n]) for n in numbers]

    def ring2(k, p):
        axis, i = orders[p][1], pos(p, 1)
        return [rcopy(k, p, 5 + step, tmid[k].at[p, (i + step) % RING], r2[k].at[p, step - 1], away(axis, step)) for step in (1, 2, 3)]

    def ring3(k, p):
        axis, i = orders[p][2], pos(p, 2)
        return [rcopy(k, p, 8 + step, umid[k].at[p, (i + step) % RING], r3[k].at[p, step - 1], away(axis, step)) for step in (1, 2, 3)]

    def stage_a(k):
        pair_copy(k).wait_recv()
        r = ROW_CHUNKS[k]

        def block(e, carry):
            ye, xe = e // RING, e % RING
            for zz in range(RING):
                for p in range(3):
                    row = (zz * 3 + p) * r
                    mine = pl.ds(pl.multiple_of(core * (12 * r) + row, 8), r)
                    value = cbuf[k % 2, e, mine, :] + drecv[k][e, row : row + r, :]
                    at = {"x": xe, "y": ye, "z": zz}
                    sums[k][p, at[orders[p][0]], at[orders[p][1]], at[orders[p][2]]] = value
            return carry

        lax.fori_loop(0, eblocks, block, 0)
        for n in range(4):
            for p in range(3):
                ring1(k, p, (n,))[0].start()

    def stage_b(k):
        for p in range(3):
            i = pos(p, 0)
            up, down = (i + 1) % RING, (i + 3) % RING
            copies = ring1(k, p, (0, 1, 4, 5))
            copies[0].wait_recv()
            sums[k][p, up, 0:2] = sums[k][p, up, 0:2] + r1m[k][p, 0]
            copies[2].start()
            copies[1].wait_recv()
            sums[k][p, down, 2:4] = sums[k][p, down, 2:4] + r1m[k][p, 1]
            copies[3].start()

    def stage_c(k):
        for p in range(3):
            i = pos(p, 0)
            for copy in ring1(k, p, (2, 3, 4, 5)):
                copy.wait_recv()
            tmid[k][p] = sums[k][p, i] + r1f[k][p, 0] + r1f[k][p, 1]
            for copy in ring2(k, p):
                copy.start()

    def stage_d(k):
        for p in range(3):
            for copy in ring2(k, p):
                copy.wait_recv()
            umid[k][p] = tmid[k][p, pos(p, 1)] + r2[k][p, 0] + r2[k][p, 1] + r2[k][p, 2]
            for copy in ring3(k, p):
                copy.start()

    def stage_e(k):
        r = ROW_CHUNKS[k]
        for p in range(3):
            for copy in ring3(k, p):
                copy.wait_recv()
            row = 88 * p + offsets[k]
            fin[row : row + r, :] = umid[k][p, pos(p, 2)] + r3[k][p, 0] + r3[k][p, 1] + r3[k][p, 2]

    stages = (matmul_chunk, stage_a, stage_b, stage_c, stage_d, stage_e)
    for turn in range(chunks + len(stages) - 1):
        for lag, stage in enumerate(stages):
            if 0 <= turn - lag < chunks:
                stage(turn - lag)

    keep = keep_ref[pl.ds(ex, 1), :].astype(jnp.float32)
    rows = d_model // 8
    whole = fin[...] * keep
    first, second = whole[0:rows, :], whole[whole.shape[0] - rows :, :]
    out_ref[...] = jnp.where(core == 0, first, second)

    for stage in range(4):
        for copy in count_copies(stage):
            copy.wait_send()
    for k in range(max(chunks - 2, 0), chunks):
        pair_copy(k).wait_send()
    for k in range(chunks):
        for p in range(3):
            for copy in ring1(k, p, range(6)) + ring2(k, p) + ring3(k, p):
                copy.wait_send()


def solution(mesh):
    devices = mesh.devices.size

    def local(tokens, router_logits, gate_grad, expert_index, keep_mask):
        tok_rows, d_model = tokens.shape
        experts = router_logits.shape[1]
        eblocks = experts // LANES
        chunks = len(ROW_CHUNKS)
        f32, bf16, i32 = jnp.float32, jnp.bfloat16, jnp.int32
        rmax = max(ROW_CHUNKS)
        vm = pltpu.VMEM

        def per_chunk(shape_of):
            return [vm(shape_of(r), f32) for r in ROW_CHUNKS]

        scratch = [
            vm((2, TB, experts), bf16),
            vm((tok_rows, LANES), i32),
            vm((tok_rows, LANES), f32),
            vm((tok_rows, LANES), f32),
            vm((tok_rows, experts), f32),
            vm((2, tok_rows, experts), bf16),
            vm((24 * sum(ROW_CHUNKS), tok_rows), bf16),
            vm((2, eblocks, 24 * rmax, LANES), f32),
            per_chunk(lambda r: (eblocks, 12 * r, LANES)),
            per_chunk(lambda r: (3, 4, 4, 4, r, LANES)),
            per_chunk(lambda r: (3, 2, 2, 4, r, LANES)),
            per_chunk(lambda r: (3, 2, 4, 4, r, LANES)),
            per_chunk(lambda r: (3, 4, 4, r, LANES)),
            per_chunk(lambda r: (3, 3, 4, r, LANES)),
            per_chunk(lambda r: (3, 4, r, LANES)),
            per_chunk(lambda r: (3, 3, r, LANES)),
            vm((264, LANES), f32),
            vm((4, eblocks, LANES), i32),
            vm((10, eblocks, LANES), i32),
            vm((eblocks, LANES), f32),
            pltpu.SemaphoreType.DMA((2,)),
            pltpu.SemaphoreType.DMA((chunks,)),
            pltpu.SemaphoreType.DMA((10,)),
            pltpu.SemaphoreType.DMA((10,)),
            pltpu.SemaphoreType.DMA((chunks,)),
            pltpu.SemaphoreType.DMA((chunks,)),
            pltpu.SemaphoreType.DMA((chunks, 3, 12)),
            pltpu.SemaphoreType.DMA((chunks, 3, 12)),
        ]
        return pl.pallas_call(
            functools.partial(kernel, tok_rows * devices),
            out_shape=jax.ShapeDtypeStruct((d_model // 8, LANES), f32),
            in_specs=[pl.BlockSpec(memory_space=pltpu.VMEM)] * 3 + [pl.BlockSpec(memory_space=pl.ANY)] * 2,
            out_specs=pl.BlockSpec(memory_space=pltpu.VMEM),
            scratch_shapes=scratch,
            compiler_params=pltpu.CompilerParams(collective_id=0, has_side_effects=True, vmem_limit_bytes=67043328),
        )(
            expert_index.reshape(tok_rows // LANES, LANES),
            gate_grad.reshape(tok_rows // LANES, LANES),
            keep_mask.reshape(eblocks, LANES),
            tokens.T,
            router_logits,
        ).T

    return jax.shard_map(
        local,
        mesh=mesh,
        in_specs=(P(("dp", "expert"), None), P(("dp", "expert"), None), P(("dp", "expert")), P(("dp", "expert"), None), P()),
        out_specs=P("expert", "dp"),
        check_vma=False,
    )
```

```python
import functools

import jax
import jax.numpy as jnp
from jax import lax
from jax.experimental import pallas as pl
from jax.experimental.pallas import tpu as pltpu
from jax.sharding import PartitionSpec as P

MESH = pl.DeviceIdType.MESH
RING = 4
LANES = 128
ROW_CHUNKS = (8, 16, 16, 16, 16, 16)
TB = 128


def kernel(total_tokens, idx_ref, gate_ref, keep_ref, tok_ref, logit_ref, out_ref,
           lbuf, icol, acol, drop, ptab, gmat, xt, cbuf, drecv, sums, r1m, r1f, tmid, r2m, r2f, umid, r3,
           fin, cnt, cnt_recv, aux_ref,
           lsem, xsem, csend, crecv, dsend, drsem, ssem, rsem):
    d_model, tok_rows = tok_ref.shape
    experts = logit_ref.shape[1]
    eblocks = experts // LANES
    blocks = tok_rows // TB
    chunks = len(ROW_CHUNKS)
    offsets = [sum(ROW_CHUNKS[:k]) for k in range(chunks)]

    dp = lax.axis_index("dp")
    ex = lax.axis_index("expert")
    zc, core = dp // 2, dp % 2
    yc, xc = ex // RING, ex % RING
    here = {"x": xc, "y": yc, "z": zc}

    def device(**moved):
        at = dict(here, **moved)
        return (2 * at["z"] + core, RING * at["y"] + at["x"])

    sibling = (2 * zc + 1 - core, ex)
    same_column = [((dp + step) % 8, ex) for step in range(1, 8)]

    def away(axis, step):
        return device(**{axis: (here[axis] + step) % RING})

    def load_logits(b, slot):
        return pltpu.make_async_copy(logit_ref.at[pl.ds(b * TB, TB), :], lbuf.at[slot], lsem.at[slot])

    for k in range(chunks):
        r = ROW_CHUNKS[k]
        for group in range(24):
            cc, zz, part = group // 12, (group // 3) % 4, group % 3
            src = (d_model // RING) * zz + 256 * cc + 88 * part + offsets[k]
            dst = 24 * offsets[k] + r * group
            pltpu.make_async_copy(tok_ref.at[pl.ds(src, r), :], xt.at[pl.ds(dst, r), :], xsem.at[k]).start()

    load_logits(0, 0).start()
    load_logits(1, 1).start()

    barrier = pltpu.get_barrier_semaphore()
    peers = same_column + [away(axis, step) for axis in "xy" for step in (1, 2, 3)]
    for peer in peers:
        pl.semaphore_signal(barrier, inc=1, device_id=peer, device_id_type=MESH)

    idx = idx_ref[...]
    total = jnp.zeros((eblocks, LANES), jnp.float32)
    for b in range(blocks):
        row = idx[b : b + 1, :]
        high = (row // LANES == lax.broadcasted_iota(jnp.int32, (eblocks, LANES), 0)).astype(jnp.bfloat16)
        low = (row % LANES == lax.broadcasted_iota(jnp.int32, (LANES, LANES), 0)).astype(jnp.bfloat16)
        total = total + lax.dot_general(high, low, (((1,), (1,)), ((), ())), preferred_element_type=jnp.float32)
    cnt[0] = total.astype(jnp.int32)

    def count_copies(stage):
        targets = same_column if stage == 0 else [away("xy"[stage - 1], step) for step in (1, 2, 3)]
        first = (0, 7, 10)[stage]
        return [
            pltpu.make_async_remote_copy(cnt.at[stage], cnt_recv.at[first + n], csend.at[stage], crecv.at[first + n], device_id=target, device_id_type=MESH)
            for n, target in enumerate(targets)
        ]

    def count_arrive(stage):
        value = cnt[stage]
        for number, copy in enumerate(count_copies(stage)):
            copy.wait_recv()
            value = value + cnt_recv[(0, 7, 10)[stage] + number]
        return value

    def count_step(stage):
        cnt[stage + 1] = count_arrive(stage)
        for copy in count_copies(stage + 1):
            copy.start()

    idx_t = jnp.transpose(idx.astype(jnp.float32))
    gate_t = jnp.transpose(gate_ref[...])
    for b in range(blocks):
        icol[b * TB : (b + 1) * TB, :] = jnp.broadcast_to(idx_t[:, b : b + 1], (TB, LANES)).astype(jnp.int32)
        acol[b * TB : (b + 1) * TB, :] = jnp.broadcast_to(gate_t[:, b : b + 1], (TB, LANES))

    RS = 32

    def lane_of(j):
        return lax.broadcasted_iota(jnp.int32, (RS, LANES), 1) + j * LANES

    def stats_block(b):
        slot = b % 2
        load_logits(b, slot).wait()

        def rows(r, carry):
            local = pl.ds(pl.multiple_of(r * RS, RS), RS)
            at = pl.ds(pl.multiple_of(b * TB + r * RS, RS), RS)
            peak = lbuf[slot, local, 0:LANES].astype(jnp.float32)
            for j in range(1, eblocks):
                peak = jnp.maximum(peak, lbuf[slot, local, j * LANES : (j + 1) * LANES].astype(jnp.float32))
            peak = jnp.max(peak, axis=1, keepdims=True)
            mass = jnp.zeros((RS, LANES), jnp.float32)
            top = jnp.zeros((RS, LANES), jnp.float32)
            chosen = icol[at, :]
            for j in range(eblocks):
                weight = jnp.exp(lbuf[slot, local, j * LANES : (j + 1) * LANES].astype(jnp.float32) - peak)
                ptab[at, j * LANES : (j + 1) * LANES] = weight
                mass = mass + weight
                top = top + jnp.where(chosen == lane_of(j), weight, 0.0)
            inverse = 1.0 / jnp.sum(mass, axis=1, keepdims=True)
            top_prob = jnp.sum(top, axis=1, keepdims=True) * inverse
            acol[at, :] = acol[at, :] * top_prob
            for j in range(eblocks):
                ptab[at, j * LANES : (j + 1) * LANES] = ptab[at, j * LANES : (j + 1) * LANES] * inverse
            return carry

        lax.fori_loop(0, TB // RS, rows, 0)

    def prep(b, carry):
        stats_block(b)

        @pl.when(b + 2 < blocks)
        def _():
            load_logits(b + 2, b % 2).start()

        return carry

    with jax.named_scope("prep_0"):
        lax.fori_loop(0, 3, prep, 0)
    with jax.named_scope("barrier"):
        pl.semaphore_wait(barrier, len(peers))
    for copy in count_copies(0):
        copy.start()
    with jax.named_scope("prep_1"):
        lax.fori_loop(3, 6, prep, 0)
    with jax.named_scope("count_step_0"):
        count_step(0)
    with jax.named_scope("prep_2"):
        lax.fori_loop(6, 8, prep, 0)
    with jax.named_scope("count_step_1"):
        count_step(1)
    with jax.named_scope("count_last"):
        aux_ref[...] = count_arrive(2).astype(jnp.float32) * (experts / total_tokens)

    def spread_rows(r, carry):
        at = pl.ds(pl.multiple_of(r * RS, RS), RS)
        acc = ptab[at, 0:LANES] * aux_ref[0:1, :]
        for j in range(1, eblocks):
            acc = acc + ptab[at, j * LANES : (j + 1) * LANES] * aux_ref[j : j + 1, :]
        drop[at, :] = jnp.sum(acc, axis=1, keepdims=True) + acol[at, :]
        return carry

    with jax.named_scope("spread"):
        lax.fori_loop(0, tok_rows // RS, spread_rows, 0, unroll=4)

    def grad_quarter(q):
        for row in range(0, tok_rows, RS):
            gain = acol[row : row + RS, :]
            less = drop[row : row + RS, :]
            chosen = icol[row : row + RS, :]
            for j in range(RING * q, RING * q + RING):
                value = ptab[row : row + RS, j * LANES : (j + 1) * LANES] * (aux_ref[j : j + 1, :] - less)
                value = jnp.where(chosen == lane_of(j), value + gain, value)
                big = value.astype(jnp.bfloat16)
                cols = slice((j - RING * q) * LANES, (j - RING * q + 1) * LANES)
                gmat[q][0, row : row + RS, cols] = big
                gmat[q][1, row : row + RS, cols] = (value - big.astype(jnp.float32)).astype(jnp.bfloat16)

    def pair_copy(k, first, count):
        rows = 12 * ROW_CHUNKS[k]
        src = cbuf.at[k % 2, pl.ds(first, count), pl.ds(pl.multiple_of((1 - core) * rows, 8), rows), :]
        return pltpu.make_async_remote_copy(
            src, drecv[k].at[pl.ds(first, count)], dsend.at[k], drsem.at[k], device_id=sibling, device_id_type=MESH)

    def matmul_quarter(k, q):
        rows = 24 * ROW_CHUNKS[k]
        base = 24 * offsets[k]
        if q == 0:
            if k >= 2:
                pair_copy(k - 2, 0, eblocks).wait_send()
            chunk_rows = xt.at[pl.ds(base, rows), :]
            pltpu.make_async_copy(chunk_rows, chunk_rows, xsem.at[k]).wait()
        left = xt[base : base + rows, :]
        value = jnp.dot(left, gmat[q][0], preferred_element_type=jnp.float32)
        value = value + jnp.dot(left, gmat[q][1], preferred_element_type=jnp.float32)
        for j in range(RING):
            cbuf[k % 2, RING * q + j, 0:rows, :] = value[:, j * LANES : (j + 1) * LANES]
        pair_copy(k, RING * q, RING).start()

    orders = ("xyz", "yzx", "zxy")

    def pos(p, stage):
        return here[orders[p][stage]]

    def around(k, p, stage, numbers):
        axis, i = orders[p][stage], pos(p, stage)
        up, down, far = (i + 1) % RING, (i + 3) % RING, (i + 2) % RING
        right, left = away(axis, 1), away(axis, 3)
        s = (sums, tmid)[stage][k].at[p]
        m = (r1m, r2m)[stage][k].at[p]
        f = (r1f, r2f)[stage][k].at[p]
        table = (
            (s.at[far, 0:2], m.at[0], 0, right),
            (s.at[far, 2:4], m.at[1], 1, left),
            (s.at[up, 2:4], f.at[0, 2:4], 2, right),
            (s.at[down, 0:2], f.at[1, 0:2], 2, left),
            (s.at[up, 0:2], f.at[0, 0:2], 2, right),
            (s.at[down, 2:4], f.at[1, 2:4], 2, left),
        )
        copies = []
        for n in numbers:
            src, dst, sem, peer = table[n]
            copies.append(pltpu.make_async_remote_copy(src, dst, ssem.at[k, stage], rsem.at[k, p, 3 * stage + sem], device_id=peer, device_id_type=MESH))
        return copies

    def last_ring(k, p):
        axis, i = orders[p][2], pos(p, 2)
        return [
            pltpu.make_async_remote_copy(
                umid[k].at[p, (i + step) % RING], r3[k].at[p, step - 1], ssem.at[k, 2], rsem.at[k, p, 6], device_id=away(axis, step), device_id_type=MESH)
            for step in (1, 2, 3)
        ]

    def taken(ref, sem):
        pltpu.make_async_copy(ref, ref, sem).wait()

    def merge(k, p, stage):
        i = pos(p, stage)
        up, down = (i + 1) % RING, (i + 3) % RING
        s, m = (sums, tmid)[stage][k], (r1m, r2m)[stage][k]
        first, second, third, fourth = around(k, p, stage, (0, 1, 4, 5))
        first.wait_recv()
        s[p, up, 0:2] = s[p, up, 0:2] + m[p, 0]
        third.start()
        second.wait_recv()
        s[p, down, 2:4] = s[p, down, 2:4] + m[p, 1]
        fourth.start()

    def stage_a(k):
        pair_copy(k, 0, eblocks).wait_recv()
        r = ROW_CHUNKS[k]

        def block(e, carry):
            ye, xe = e // RING, e % RING
            for zz in range(RING):
                for p in range(3):
                    row = (zz * 3 + p) * r
                    mine = pl.ds(pl.multiple_of(core * (12 * r) + row, 8), r)
                    value = cbuf[k % 2, e, mine, :] + drecv[k][e, row : row + r, :]
                    at = {"x": xe, "y": ye, "z": zz}
                    sums[k][p, at[orders[p][0]], at[orders[p][1]], at[orders[p][2]]] = value
            return carry

        lax.fori_loop(0, eblocks, block, 0)
        for n in range(4):
            for p in range(3):
                around(k, p, 0, (n,))[0].start()

    def stage_b(k):
        for p in range(3):
            merge(k, p, 0)

    def stage_c(k):
        for p in range(3):
            taken(r1f[k].at[p], rsem.at[k, p, 2])
            tmid[k][p] = sums[k][p, pos(p, 0)] + r1f[k][p, 0] + r1f[k][p, 1]
            for copy in around(k, p, 1, (0, 1, 2, 3)):
                copy.start()

    def stage_d(k):
        for p in range(3):
            merge(k, p, 1)

    def stage_e(k):
        for p in range(3):
            taken(r2f[k].at[p], rsem.at[k, p, 5])
            umid[k][p] = tmid[k][p, pos(p, 1)] + r2f[k][p, 0] + r2f[k][p, 1]
            for copy in last_ring(k, p):
                copy.start()
        taken(sums[k].at[:, 0:3], ssem.at[k, 0])

    def stage_f(k):
        r = ROW_CHUNKS[k]
        for p in range(3):
            taken(r3[k].at[p], rsem.at[k, p, 6])
            row = 88 * p + offsets[k]
            fin[row : row + r, :] = umid[k][p, pos(p, 2)] + r3[k][p, 0] + r3[k][p, 1] + r3[k][p, 2]
        taken(tmid[k].at[:, 0:3], ssem.at[k, 1])

    plan = []
    for k in range(chunks):
        for q in range(RING):
            plan.append((RING * k + q, -1, k, "matmul", functools.partial(matmul_quarter, k, q)))
        for order, (stage, lag) in enumerate(((stage_a, 2), (stage_b, 5), (stage_c, 9), (stage_d, 12), (stage_e, 15), (stage_f, 18))):
            plan.append((RING * k + 3 + lag, order, k, stage.__name__, functools.partial(stage, k)))
    with jax.named_scope("first_chunk"):
        for q in range(RING):
            grad_quarter(q)
            if q:
                matmul_quarter(0, q - 1)
        matmul_quarter(0, RING - 1)
    for when, order, k, name, step in sorted(plan, key=lambda entry: entry[:3]):
        if when >= RING:
            with jax.named_scope(f"{name}_{k}"):
                step()

    keep = keep_ref[pl.ds(ex, 1), :].astype(jnp.float32)
    rows = d_model // 8
    whole = fin[...] * keep
    first, second = whole[0:rows, :], whole[whole.shape[0] - rows :, :]
    out_ref[...] = jnp.where(core == 0, first, second)

    taken(cnt_recv.at[0:7], csend.at[0])
    taken(cnt_recv.at[0:3], csend.at[1])
    taken(cnt_recv.at[0:3], csend.at[2])
    for k in range(max(chunks - 2, 0), chunks):
        pair_copy(k, 0, eblocks).wait_send()
    for k in range(chunks):
        taken(umid[k].at[:, 0:3], ssem.at[k, 2])


def solution(mesh):
    devices = mesh.devices.size

    def local(tokens, router_logits, gate_grad, expert_index, keep_mask):
        tok_rows, d_model = tokens.shape
        experts = router_logits.shape[1]
        eblocks = experts // LANES
        chunks = len(ROW_CHUNKS)
        f32, bf16, i32 = jnp.float32, jnp.bfloat16, jnp.int32
        rmax = max(ROW_CHUNKS)
        vm = pltpu.VMEM

        def per_chunk(shape_of):
            return [vm(shape_of(r), f32) for r in ROW_CHUNKS]

        scratch = [
            vm((2, TB, experts), bf16),
            vm((tok_rows, LANES), i32),
            vm((tok_rows, LANES), f32),
            vm((tok_rows, LANES), f32),
            vm((tok_rows, experts), f32),
            [vm((2, tok_rows, experts // RING), bf16)] * RING,
            vm((24 * sum(ROW_CHUNKS), tok_rows), bf16),
            vm((2, eblocks, 24 * rmax, LANES), f32),
            per_chunk(lambda r: (eblocks, 12 * r, LANES)),
            per_chunk(lambda r: (3, 4, 4, 4, r, LANES)),
            per_chunk(lambda r: (3, 2, 2, 4, r, LANES)),
            per_chunk(lambda r: (3, 2, 4, 4, r, LANES)),
            per_chunk(lambda r: (3, 4, 4, r, LANES)),
            per_chunk(lambda r: (3, 2, 2, r, LANES)),
            per_chunk(lambda r: (3, 2, 4, r, LANES)),
            per_chunk(lambda r: (3, 4, r, LANES)),
            per_chunk(lambda r: (3, 3, r, LANES)),
            vm((264, LANES), f32),
            vm((3, eblocks, LANES), i32),
            vm((13, eblocks, LANES), i32),
            vm((eblocks, LANES), f32),
            pltpu.SemaphoreType.DMA((2,)),
            pltpu.SemaphoreType.DMA((chunks,)),
            pltpu.SemaphoreType.DMA((3,)),
            pltpu.SemaphoreType.DMA((13,)),
            pltpu.SemaphoreType.DMA((chunks,)),
            pltpu.SemaphoreType.DMA((chunks,)),
            pltpu.SemaphoreType.DMA((chunks, 3)),
            pltpu.SemaphoreType.DMA((chunks, 3, 7)),
        ]
        return pl.pallas_call(
            functools.partial(kernel, tok_rows * devices),
            out_shape=jax.ShapeDtypeStruct((d_model // 8, LANES), f32),
            in_specs=[pl.BlockSpec(memory_space=pltpu.VMEM)] * 3 + [pl.BlockSpec(memory_space=pl.ANY)] * 2,
            out_specs=pl.BlockSpec(memory_space=pltpu.VMEM),
            scratch_shapes=scratch,
            compiler_params=pltpu.CompilerParams(collective_id=0, has_side_effects=True, vmem_limit_bytes=67043328),
        )(
            expert_index.reshape(tok_rows // LANES, LANES),
            gate_grad.reshape(tok_rows // LANES, LANES),
            keep_mask.reshape(eblocks, LANES),
            tokens.T,
            router_logits,
        ).T

    return jax.shard_map(
        local,
        mesh=mesh,
        in_specs=(P(("dp", "expert"), None), P(("dp", "expert"), None), P(("dp", "expert")), P(("dp", "expert"), None), P()),
        out_specs=P("expert", "dp"),
        check_vma=False,
    )
```

```python
import functools

import jax
import jax.numpy as jnp
from jax import lax
from jax.experimental import pallas as pl
from jax.experimental.pallas import tpu as pltpu
from jax.sharding import PartitionSpec as P

MESH = pl.DeviceIdType.MESH
RING = 4
PAIR_TIME, HOP_TIME, QUARTER_TIME = 1.5, 2.4, 0.0606
PLANE = (5, 6)
EARLY_OWN = 6
LANES = 128
ROW_CHUNKS = (8, 8, 16, 16, 16, 16, 8)
TB = 128
SLOTS = 3


def kernel(total_tokens, idx_ref, gate_ref, keep_ref, tok_ref, logit_ref, out_ref,
           lbuf, icol, acol, drop, ptab, gmat, xt, cbuf, drecv, sums, r1m, r1f, tmid, r2m, r2f, umid, r3, plane,
           fin, cnt, cnt_recv, aux_ref,
           lsem, xsem, csend, crecv, dsend, drsem, ssem, rsem):
    d_model, tok_rows = tok_ref.shape
    experts = logit_ref.shape[1]
    eblocks = experts // LANES
    blocks = tok_rows // TB
    chunks = len(ROW_CHUNKS)
    offsets = [sum(ROW_CHUNKS[:k]) for k in range(chunks)]

    dp = lax.axis_index("dp")
    ex = lax.axis_index("expert")
    zc, core = dp // 2, dp % 2
    yc, xc = ex // RING, ex % RING
    here = {"x": xc, "y": yc, "z": zc}

    def device(**moved):
        at = dict(here, **moved)
        return (2 * at["z"] + core, RING * at["y"] + at["x"])

    sibling = (2 * zc + 1 - core, ex)
    same_column = [((dp + step) % 8, ex) for step in range(1, 8)]

    def away(axis, step):
        return device(**{axis: (here[axis] + step) % RING})

    def load_logits(b, slot):
        return pltpu.make_async_copy(logit_ref.at[pl.ds(b * TB, TB), :], lbuf.at[slot], lsem.at[slot])

    for b in range(SLOTS):
        load_logits(b, b).start()

    barrier = pltpu.get_barrier_semaphore()
    peers = same_column + [away(axis, step) for axis in "xy" for step in (1, 2, 3)]
    for peer in peers:
        pl.semaphore_signal(barrier, inc=1, device_id=peer, device_id_type=MESH)

    idx = idx_ref[...]
    total = jnp.zeros((eblocks, LANES), jnp.float32)
    for b in range(blocks):
        row = idx[b : b + 1, :]
        high = (row // LANES == lax.broadcasted_iota(jnp.int32, (eblocks, LANES), 0)).astype(jnp.bfloat16)
        low = (row % LANES == lax.broadcasted_iota(jnp.int32, (LANES, LANES), 0)).astype(jnp.bfloat16)
        total = total + lax.dot_general(high, low, (((1,), (1,)), ((), ())), preferred_element_type=jnp.float32)
    cnt[0] = total.astype(jnp.int32)

    def count_copies(stage):
        targets = same_column if stage == 0 else [away("xy"[stage - 1], step) for step in (1, 2, 3)]
        first = (0, 7, 10)[stage]
        return [
            pltpu.make_async_remote_copy(cnt.at[stage], cnt_recv.at[first + n], csend.at[stage], crecv.at[first + n], device_id=target, device_id_type=MESH)
            for n, target in enumerate(targets)
        ]

    def count_arrive(stage):
        value = cnt[stage]
        for number, copy in enumerate(count_copies(stage)):
            copy.wait_recv()
            value = value + cnt_recv[(0, 7, 10)[stage] + number]
        return value

    def count_step(stage):
        cnt[stage + 1] = count_arrive(stage)
        for copy in count_copies(stage + 1):
            copy.start()

    idx_t = jnp.transpose(idx.astype(jnp.float32))
    gate_t = jnp.transpose(gate_ref[...])
    for b in range(blocks):
        icol[b * TB : (b + 1) * TB, :] = jnp.broadcast_to(idx_t[:, b : b + 1], (TB, LANES)).astype(jnp.int32)
        acol[b * TB : (b + 1) * TB, :] = jnp.broadcast_to(gate_t[:, b : b + 1], (TB, LANES))

    RS = 32

    def lane_of(j):
        return lax.broadcasted_iota(jnp.int32, (RS, LANES), 1) + j * LANES

    def stats_block(b):
        slot = b % SLOTS
        load_logits(b, slot).wait()

        def rows(r, carry):
            local = pl.ds(pl.multiple_of(r * RS, RS), RS)
            at = pl.ds(pl.multiple_of(b * TB + r * RS, RS), RS)
            peak = lbuf[slot, local, 0:LANES].astype(jnp.float32)
            for j in range(1, eblocks):
                peak = jnp.maximum(peak, lbuf[slot, local, j * LANES : (j + 1) * LANES].astype(jnp.float32))
            peak = jnp.max(peak, axis=1, keepdims=True)
            mass = jnp.zeros((RS, LANES), jnp.float32)
            top = jnp.zeros((RS, LANES), jnp.float32)
            chosen = icol[at, :]
            for j in range(eblocks):
                weight = jnp.exp(lbuf[slot, local, j * LANES : (j + 1) * LANES].astype(jnp.float32) - peak)
                ptab[at, j * LANES : (j + 1) * LANES] = weight
                mass = mass + weight
                top = top + jnp.where(chosen == lane_of(j), weight, 0.0)
            inverse = 1.0 / jnp.sum(mass, axis=1, keepdims=True)
            top_prob = jnp.sum(top, axis=1, keepdims=True) * inverse
            acol[at, :] = acol[at, :] * top_prob
            for j in range(eblocks):
                ptab[at, j * LANES : (j + 1) * LANES] = ptab[at, j * LANES : (j + 1) * LANES] * inverse
            return carry

        lax.fori_loop(0, TB // RS, rows, 0)

    def prep(b, carry):
        stats_block(b)

        @pl.when(b + SLOTS < blocks)
        def _():
            load_logits(b + SLOTS, b % SLOTS).start()

        return carry

    with jax.named_scope("prep_0"):
        lax.fori_loop(0, 2, prep, 0)
    with jax.named_scope("barrier"):
        pl.semaphore_wait(barrier, len(peers))
    for copy in count_copies(0):
        copy.start()

    for k in range(chunks):
        r = ROW_CHUNKS[k]
        for group in range(24):
            cc, zz, part = group // 12, (group // 3) % 4, group % 3
            src = (d_model // RING) * zz + 256 * cc + 88 * part + offsets[k]
            dst = 24 * offsets[k] + r * group
            pltpu.make_async_copy(tok_ref.at[pl.ds(src, r), :], xt.at[pl.ds(dst, r), :], xsem.at[k]).start()

    with jax.named_scope("prep_1"):
        lax.fori_loop(2, 5, prep, 0)
    with jax.named_scope("count_step_0"):
        count_step(0)
    with jax.named_scope("prep_2"):
        lax.fori_loop(5, 8, prep, 0)
    with jax.named_scope("count_step_1"):
        count_step(1)
    with jax.named_scope("count_last"):
        aux_ref[...] = count_arrive(2).astype(jnp.float32) * (experts / total_tokens)

    def spread_rows(r, carry):
        at = pl.ds(pl.multiple_of(r * RS, RS), RS)
        acc = ptab[at, 0:LANES] * aux_ref[0:1, :]
        for j in range(1, eblocks):
            acc = acc + ptab[at, j * LANES : (j + 1) * LANES] * aux_ref[j : j + 1, :]
        drop[at, :] = jnp.sum(acc, axis=1, keepdims=True) + acol[at, :]
        return carry

    with jax.named_scope("spread"):
        lax.fori_loop(0, tok_rows // RS, spread_rows, 0, unroll=8)

    def grad_piece(q, row):
        gain = acol[row : row + RS, :]
        less = drop[row : row + RS, :]
        chosen = icol[row : row + RS, :]
        for j in range(RING * q, RING * q + RING):
            value = ptab[row : row + RS, j * LANES : (j + 1) * LANES] * (aux_ref[j : j + 1, :] - less)
            value = jnp.where(chosen == lane_of(j), value + gain, value)
            big = value.astype(jnp.bfloat16)
            cols = slice((j - RING * q) * LANES, (j - RING * q + 1) * LANES)
            gmat[q][0, row : row + RS, cols] = big
            gmat[q][1, row : row + RS, cols] = (value - big.astype(jnp.float32)).astype(jnp.bfloat16)

    def pair_copy(k, first, count):
        rows = 12 * ROW_CHUNKS[k]
        src = cbuf.at[k % 2, pl.ds(first, count), pl.ds(pl.multiple_of((1 - core) * rows, 8), rows), :]
        return pltpu.make_async_remote_copy(
            src, drecv[k].at[pl.ds(first, count)], dsend.at[k], drsem.at[k], device_id=sibling, device_id_type=MESH)

    NT, KT = 256, 256

    def matmul_quarter(k, q, beside=()):
        rows = 24 * ROW_CHUNKS[k]
        base = 24 * offsets[k]
        if q == 0:
            if k >= 2:
                pair_copy(k - 2, 0, eblocks).wait_send()
            chunk_rows = xt.at[pl.ds(base, rows), :]
            pltpu.make_async_copy(chunk_rows, chunk_rows, xsem.at[k]).wait()
        count = experts // RING // NT * 2 * (tok_rows // KT)
        beside = list(beside)
        each = -(-len(beside) // count)
        for n in range(experts // RING // NT):
            value = None
            for half in range(2):
                for kt in range(tok_rows // KT):
                    part = jnp.dot(
                        xt[base : base + rows, kt * KT : (kt + 1) * KT],
                        gmat[q][half, kt * KT : (kt + 1) * KT, n * NT : (n + 1) * NT],
                        preferred_element_type=jnp.float32)
                    value = part if value is None else value + part
                    for piece in beside[:each]:
                        piece()
                    beside = beside[each:]
            for j in range(NT // LANES):
                cbuf[k % 2, RING * q + n * (NT // LANES) + j, 0:rows, :] = value[:, j * LANES : (j + 1) * LANES]
        pair_copy(k, RING * q, RING).start()

    orders = ("xyz", "yzx", "zxy")

    def pos(p, stage):
        return here[orders[p][stage]]

    def around(k, p, stage, numbers):
        axis, i = orders[p][stage], pos(p, stage)
        up, down, far = (i + 1) % RING, (i + 3) % RING, (i + 2) % RING
        right, left = away(axis, 1), away(axis, 3)
        s = (sums, tmid)[stage][k].at[p]
        m = (r1m, r2m)[stage][k].at[p]
        f = (r1f, r2f)[stage][k].at[p]
        table = (
            (s.at[far, 0:2], m.at[0], 0, right),
            (s.at[far, 2:4], m.at[1], 1, left),
            (s.at[up, 2:4], f.at[0, 2:4], 2, right),
            (s.at[down, 0:2], f.at[1, 0:2], 2, left),
            (s.at[up, 0:2], f.at[0, 0:2], 2, right),
            (s.at[down, 2:4], f.at[1, 2:4], 2, left),
            (s.at[up], f.at[0], 2, right),
            (s.at[down], f.at[1], 2, left),
        )
        copies = []
        for n in numbers:
            src, dst, sem, peer = table[n]
            copies.append(pltpu.make_async_remote_copy(src, dst, ssem.at[k, stage], rsem.at[k, p, 3 * stage + sem], device_id=peer, device_id_type=MESH))
        return copies

    def last_ring(k, p):
        axis, i = orders[p][2], pos(p, 2)
        return [
            pltpu.make_async_remote_copy(
                umid[k].at[p, (i + step) % RING], r3[k].at[p, step - 1], ssem.at[k, 2], rsem.at[k, p, 6], device_id=away(axis, step), device_id_type=MESH)
            for step in (1, 2, 3)
        ]

    def taken(ref, sem):
        pltpu.make_async_copy(ref, ref, sem).wait()

    def merge(k, p, stage):
        i = pos(p, stage)
        up, down = (i + 1) % RING, (i + 3) % RING
        s, m = (sums, tmid)[stage][k], (r1m, r2m)[stage][k]
        early = stage == 0 and k < EARLY_OWN
        first, second, third, fourth = around(k, p, stage, (0, 1, 4, 5) if early else (0, 1, 6, 7))
        first.wait_recv()
        s[p, up, 0:2] = s[p, up, 0:2] + m[p, 0]
        third.start()
        second.wait_recv()
        s[p, down, 2:4] = s[p, down, 2:4] + m[p, 1]
        fourth.start()

    def stage_a(k):
        pair_copy(k, 0, eblocks).wait_recv()
        r = ROW_CHUNKS[k]

        def block(e, carry):
            ye, xe = e // RING, e % RING
            for zz in range(RING):
                for p in range(3):
                    row = (zz * 3 + p) * r
                    mine = pl.ds(pl.multiple_of(core * (12 * r) + row, 8), r)
                    value = cbuf[k % 2, e, mine, :] + drecv[k][e, row : row + r, :]
                    at = {"x": xe, "y": ye, "z": zz}
                    sums[k][p, at[orders[p][0]], at[orders[p][1]], at[orders[p][2]]] = value
            return carry

        lax.fori_loop(0, eblocks, block, 0)
        for n in range(4 if k < EARLY_OWN else 2):
            for p in range(3):
                around(k, p, 0, (n,))[0].start()

    def stage_b(k):
        for p in range(3):
            merge(k, p, 0)

    def stage_c(k):
        for p in range(3):
            taken(r1f[k].at[p], rsem.at[k, p, 2])
            tmid[k][p] = sums[k][p, pos(p, 0)] + r1f[k][p, 0] + r1f[k][p, 1]
            for copy in around(k, p, 1, (0, 1)):
                copy.start()

    def stage_d(k):
        for p in range(3):
            merge(k, p, 1)

    def stage_e(k):
        for p in range(3):
            taken(r2f[k].at[p], rsem.at[k, p, 5])
            umid[k][p] = tmid[k][p, pos(p, 1)] + r2f[k][p, 0] + r2f[k][p, 1]
            for copy in last_ring(k, p):
                copy.start()
        taken(sums[k].at[:, 0:3], ssem.at[k, 0])

    def stage_f(k):
        r = ROW_CHUNKS[k]
        for p in range(3):
            taken(r3[k].at[p], rsem.at[k, p, 6])
            row = 88 * p + offsets[k]
            fin[row : row + r, :] = umid[k][p, pos(p, 2)] + r3[k][p, 0] + r3[k][p, 1] + r3[k][p, 2]
        taken(tmid[k].at[:, 0:3], ssem.at[k, 1])

    def plane_ring(k, p):
        (one, i), (two, j) = (orders[p][1], pos(p, 1)), (orders[p][2], pos(p, 2))
        copies = []
        for n in range(1, RING * RING):
            b, c = (i + n // RING) % RING, (j + n % RING) % RING
            copies.append(pltpu.make_async_remote_copy(
                tmid[k].at[p, b, c], plane[k].at[p, n - 1], ssem.at[k, 2], rsem.at[k, p, 6], device_id=device(**{one: b, two: c}), device_id_type=MESH))
        return copies

    def stage_plane(k):
        for p in range(3):
            taken(r1f[k].at[p], rsem.at[k, p, 2])
            tmid[k][p] = sums[k][p, pos(p, 0)] + r1f[k][p, 0] + r1f[k][p, 1]
            for copy in plane_ring(k, p):
                copy.start()
        taken(sums[k].at[:, 0:3], ssem.at[k, 0])

    def stage_g(k):
        r = ROW_CHUNKS[k]
        for p in range(3):
            taken(plane[k].at[p], rsem.at[k, p, 6])
            row = 88 * p + offsets[k]
            value = tmid[k][p, pos(p, 1), pos(p, 2)]
            for n in range(RING * RING - 1):
                value = value + plane[k][p, n]
            fin[row : row + r, :] = value

    def grad_pieces(q):
        return [functools.partial(grad_piece, q, row) for row in range(0, tok_rows, RS)]

    with jax.named_scope("first_chunk"):
        for piece in grad_pieces(0):
            piece()
        for q in range(RING):
            matmul_quarter(0, q, grad_pieces(q + 1) if q + 1 < RING else ())

    ring_stages = ((stage_a, 0.0), (stage_b, 0.088), (stage_c, 0.022), (stage_d, 0.044), (stage_e, 0.033), (stage_f, 0.0))
    plane_stages = ((stage_a, 0.0), (stage_b, 0.088), (stage_plane, 0.175), (stage_g, 0.0))
    quarters = [(k, q) for k in range(1, chunks) for q in range(RING)]
    ready = [(PAIR_TIME, 0, 0)]
    clock, links = 0.0, 0.0
    while quarters or ready:
        ready.sort()
        if ready and (ready[0][0] <= clock or not quarters):
            when, k, number = ready.pop(0)
            stages = plane_stages if k in PLANE else ring_stages
            stage, wire = stages[number]
            r = ROW_CHUNKS[k]
            clock = max(clock, when) + (0.04 if number else 0.025 * r)
            with jax.named_scope(f"{stage.__name__}_{k}"):
                stage(k)
            if number == 0:
                arrival = max(clock, links) + 0.088 * r
                links = arrival + (0.088 * r if k < EARLY_OWN else 0.0)
            else:
                arrival = links = max(clock, links) + wire * r * (1 if number > 1 or k < EARLY_OWN else 2)
            if number + 1 < len(stages):
                ready.append((arrival + HOP_TIME + (1.5 if stage is stage_plane else 0.0), k, number + 1))
        else:
            k, q = quarters.pop(0)
            with jax.named_scope(f"matmul_{k}"):
                matmul_quarter(k, q)
            clock += QUARTER_TIME * ROW_CHUNKS[k]
            if q == RING - 1:
                ready.append((clock + PAIR_TIME, k, 0))

    keep = keep_ref[pl.ds(ex, 1), :].astype(jnp.float32)
    rows = d_model // 8
    whole = fin[...] * keep
    first, second = whole[0:rows, :], whole[whole.shape[0] - rows :, :]
    out_ref[...] = jnp.where(core == 0, first, second)

    taken(cnt_recv.at[0:7], csend.at[0])
    taken(cnt_recv.at[0:3], csend.at[1])
    taken(cnt_recv.at[0:3], csend.at[2])
    for k in range(max(chunks - 2, 0), chunks):
        pair_copy(k, 0, eblocks).wait_send()
    for k in range(chunks):
        taken(plane[k] if k in PLANE else umid[k].at[:, 0:3], ssem.at[k, 2])


def solution(mesh):
    devices = mesh.devices.size

    def local(tokens, router_logits, gate_grad, expert_index, keep_mask):
        tok_rows, d_model = tokens.shape
        experts = router_logits.shape[1]
        eblocks = experts // LANES
        chunks = len(ROW_CHUNKS)
        f32, bf16, i32 = jnp.float32, jnp.bfloat16, jnp.int32
        rmax = max(ROW_CHUNKS)
        vm = pltpu.VMEM

        def per_chunk(shape_of):
            return [vm(shape_of(r), f32) for r in ROW_CHUNKS]

        scratch = [
            vm((SLOTS, TB, experts), bf16),
            vm((tok_rows, LANES), i32),
            vm((tok_rows, LANES), f32),
            vm((tok_rows, LANES), f32),
            vm((tok_rows, experts), f32),
            [vm((2, tok_rows, experts // RING), bf16)] * RING,
            vm((24 * sum(ROW_CHUNKS), tok_rows), bf16),
            vm((2, eblocks, 24 * rmax, LANES), f32),
            per_chunk(lambda r: (eblocks, 12 * r, LANES)),
            per_chunk(lambda r: (3, 4, 4, 4, r, LANES)),
            per_chunk(lambda r: (3, 2, 2, 4, r, LANES)),
            per_chunk(lambda r: (3, 2, 4, 4, r, LANES)),
            per_chunk(lambda r: (3, 4, 4, r, LANES)),
            per_chunk(lambda r: (3, 2, 2, r, LANES)),
            per_chunk(lambda r: (3, 2, 4, r, LANES)),
            per_chunk(lambda r: (3, 4, r, LANES)),
            per_chunk(lambda r: (3, 3, r, LANES)),
            [vm((3, RING * RING - 1, r if k in PLANE else 8, LANES), f32) for k, r in enumerate(ROW_CHUNKS)],
            vm((264, LANES), f32),
            vm((3, eblocks, LANES), i32),
            vm((13, eblocks, LANES), i32),
            vm((eblocks, LANES), f32),
            pltpu.SemaphoreType.DMA((SLOTS,)),
            pltpu.SemaphoreType.DMA((chunks,)),
            pltpu.SemaphoreType.DMA((3,)),
            pltpu.SemaphoreType.DMA((13,)),
            pltpu.SemaphoreType.DMA((chunks,)),
            pltpu.SemaphoreType.DMA((chunks,)),
            pltpu.SemaphoreType.DMA((chunks, 3)),
            pltpu.SemaphoreType.DMA((chunks, 3, 7)),
        ]
        return pl.pallas_call(
            functools.partial(kernel, tok_rows * devices),
            out_shape=jax.ShapeDtypeStruct((d_model // 8, LANES), f32),
            in_specs=[pl.BlockSpec(memory_space=pltpu.VMEM)] * 3 + [pl.BlockSpec(memory_space=pl.ANY)] * 2,
            out_specs=pl.BlockSpec(memory_space=pltpu.VMEM),
            scratch_shapes=scratch,
            compiler_params=pltpu.CompilerParams(collective_id=0, has_side_effects=True, vmem_limit_bytes=67043328),
        )(
            expert_index.reshape(tok_rows // LANES, LANES),
            gate_grad.reshape(tok_rows // LANES, LANES),
            keep_mask.reshape(eblocks, LANES),
            tokens.T,
            router_logits,
        ).T

    return jax.shard_map(
        local,
        mesh=mesh,
        in_specs=(P(("dp", "expert"), None), P(("dp", "expert"), None), P(("dp", "expert")), P(("dp", "expert"), None), P()),
        out_specs=P("expert", "dp"),
        check_vma=False,
    )
```

```python
import functools

import jax
import jax.numpy as jnp
from jax import lax
from jax.experimental import pallas as pl
from jax.experimental.pallas import tpu as pltpu
from jax.sharding import PartitionSpec as P

MESH = pl.DeviceIdType.MESH
RING = 4
LOW = jnp.float8_e5m2
PAIR_TIME, HOP_TIME, QUARTER_TIME = 1.1, 2.4, 0.046
PLANE = (5, 6)
EARLY_OWN = 6
LANES = 128
ROW_CHUNKS = (8, 8, 16, 16, 16, 16, 8)
TB = 128
SLOTS = 3


def kernel(total_tokens, idx_ref, gate_ref, keep_ref, tok_ref, logit_ref, out_ref,
           lbuf, icol, acol, drop, ptab, gmat, glow, xt, xlow, cbuf, drecv, sums, r1m, r1f, tmid, r2m, r2f, umid, r3, plane,
           fin, cnt, cnt_recv, aux_ref,
           lsem, xsem, csend, crecv, dsend, drsem, ssem, rsem):
    d_model, tok_rows = tok_ref.shape
    experts = logit_ref.shape[1]
    eblocks = experts // LANES
    blocks = tok_rows // TB
    chunks = len(ROW_CHUNKS)
    offsets = [sum(ROW_CHUNKS[:k]) for k in range(chunks)]

    dp = lax.axis_index("dp")
    ex = lax.axis_index("expert")
    zc, core = dp // 2, dp % 2
    yc, xc = ex // RING, ex % RING
    here = {"x": xc, "y": yc, "z": zc}

    def device(**moved):
        at = dict(here, **moved)
        return (2 * at["z"] + core, RING * at["y"] + at["x"])

    sibling = (2 * zc + 1 - core, ex)
    same_column = [((dp + step) % 8, ex) for step in range(1, 8)]

    def away(axis, step):
        return device(**{axis: (here[axis] + step) % RING})

    def load_logits(b, slot):
        return pltpu.make_async_copy(logit_ref.at[pl.ds(b * TB, TB), :], lbuf.at[slot], lsem.at[slot])

    for b in range(SLOTS):
        load_logits(b, b).start()

    barrier = pltpu.get_barrier_semaphore()
    peers = same_column + [away(axis, step) for axis in "xy" for step in (1, 2, 3)]
    for peer in peers:
        pl.semaphore_signal(barrier, inc=1, device_id=peer, device_id_type=MESH)

    idx = idx_ref[...]
    total = jnp.zeros((eblocks, LANES), jnp.float32)
    for b in range(blocks):
        row = idx[b : b + 1, :]
        high = (row // LANES == lax.broadcasted_iota(jnp.int32, (eblocks, LANES), 0)).astype(jnp.bfloat16)
        low = (row % LANES == lax.broadcasted_iota(jnp.int32, (LANES, LANES), 0)).astype(jnp.bfloat16)
        total = total + lax.dot_general(high, low, (((1,), (1,)), ((), ())), preferred_element_type=jnp.float32)
    cnt[0] = total.astype(jnp.int32)

    def count_copies(stage):
        targets = same_column if stage == 0 else [away("xy"[stage - 1], step) for step in (1, 2, 3)]
        first = (0, 7, 10)[stage]
        return [
            pltpu.make_async_remote_copy(cnt.at[stage], cnt_recv.at[first + n], csend.at[stage], crecv.at[first + n], device_id=target, device_id_type=MESH)
            for n, target in enumerate(targets)
        ]

    def count_arrive(stage):
        value = cnt[stage]
        for number, copy in enumerate(count_copies(stage)):
            copy.wait_recv()
            value = value + cnt_recv[(0, 7, 10)[stage] + number]
        return value

    def count_step(stage):
        cnt[stage + 1] = count_arrive(stage)
        for copy in count_copies(stage + 1):
            copy.start()

    idx_t = jnp.transpose(idx.astype(jnp.float32))
    gate_t = jnp.transpose(gate_ref[...])
    for b in range(blocks):
        icol[b * TB : (b + 1) * TB, :] = jnp.broadcast_to(idx_t[:, b : b + 1], (TB, LANES)).astype(jnp.int32)
        acol[b * TB : (b + 1) * TB, :] = jnp.broadcast_to(gate_t[:, b : b + 1], (TB, LANES))

    RS = 32

    def lane_of(j):
        return lax.broadcasted_iota(jnp.int32, (RS, LANES), 1) + j * LANES

    def stats_block(b):
        slot = b % SLOTS
        load_logits(b, slot).wait()

        def rows(r, carry):
            local = pl.ds(pl.multiple_of(r * RS, RS), RS)
            at = pl.ds(pl.multiple_of(b * TB + r * RS, RS), RS)
            peak = lbuf[slot, local, 0:LANES].astype(jnp.float32)
            for j in range(1, eblocks):
                peak = jnp.maximum(peak, lbuf[slot, local, j * LANES : (j + 1) * LANES].astype(jnp.float32))
            peak = jnp.max(peak, axis=1, keepdims=True)
            mass = jnp.zeros((RS, LANES), jnp.float32)
            top = jnp.zeros((RS, LANES), jnp.float32)
            chosen = icol[at, :]
            for j in range(eblocks):
                weight = jnp.exp(lbuf[slot, local, j * LANES : (j + 1) * LANES].astype(jnp.float32) - peak)
                ptab[at, j * LANES : (j + 1) * LANES] = weight
                mass = mass + weight
                top = top + jnp.where(chosen == lane_of(j), weight, 0.0)
            inverse = 1.0 / jnp.sum(mass, axis=1, keepdims=True)
            top_prob = jnp.sum(top, axis=1, keepdims=True) * inverse
            acol[at, :] = acol[at, :] * top_prob
            for j in range(eblocks):
                ptab[at, j * LANES : (j + 1) * LANES] = ptab[at, j * LANES : (j + 1) * LANES] * inverse
            return carry

        lax.fori_loop(0, TB // RS, rows, 0)

    def prep(b, carry):
        stats_block(b)

        @pl.when(b + SLOTS < blocks)
        def _():
            load_logits(b + SLOTS, b % SLOTS).start()

        return carry

    with jax.named_scope("prep_0"):
        lax.fori_loop(0, 2, prep, 0)
    with jax.named_scope("barrier"):
        pl.semaphore_wait(barrier, len(peers))
    for copy in count_copies(0):
        copy.start()

    for k in range(chunks):
        r = ROW_CHUNKS[k]
        for group in range(24):
            cc, zz, part = group // 12, (group // 3) % 4, group % 3
            src = (d_model // RING) * zz + 256 * cc + 88 * part + offsets[k]
            dst = 24 * offsets[k] + r * group
            pltpu.make_async_copy(tok_ref.at[pl.ds(src, r), :], xt.at[pl.ds(dst, r), :], xsem.at[k]).start()

    with jax.named_scope("prep_1"):
        lax.fori_loop(2, 5, prep, 0)
    with jax.named_scope("count_step_0"):
        count_step(0)
    with jax.named_scope("prep_2"):
        lax.fori_loop(5, 8, prep, 0)
    with jax.named_scope("count_step_1"):
        count_step(1)
    def lower_rows(n, carry):
        at = pl.ds(pl.multiple_of(n * LR, LR), LR)
        xlow[at, :] = xt[at, :].astype(LOW)
        return carry

    LR = 96
    with jax.named_scope("lower"):
        for k in range(chunks):
            chunk_rows = xt.at[pl.ds(24 * offsets[k], 24 * ROW_CHUNKS[k]), :]
            pltpu.make_async_copy(chunk_rows, chunk_rows, xsem.at[k]).wait()
        lax.fori_loop(0, 24 * sum(ROW_CHUNKS) // LR, lower_rows, 0)

    with jax.named_scope("count_last"):
        raw = count_arrive(2).astype(jnp.float32) * (experts / total_tokens)
        scale = 4194304.0 / (jnp.max(jnp.max(raw, axis=1, keepdims=True), axis=0, keepdims=True) + 6.0)
        aux_ref[...] = raw * scale

    def spread_rows(r, carry):
        at = pl.ds(pl.multiple_of(r * RS, RS), RS)
        acc = ptab[at, 0:LANES] * aux_ref[0:1, :]
        for j in range(1, eblocks):
            acc = acc + ptab[at, j * LANES : (j + 1) * LANES] * aux_ref[j : j + 1, :]
        gain = acol[at, :] * scale
        acol[at, :] = gain
        drop[at, :] = jnp.sum(acc, axis=1, keepdims=True) + gain
        return carry

    with jax.named_scope("spread"):
        lax.fori_loop(0, tok_rows // RS, spread_rows, 0, unroll=8)

    def grad_piece(q, row):
        gain = acol[row : row + RS, :]
        less = drop[row : row + RS, :]
        chosen = icol[row : row + RS, :]
        for j in range(RING * q, RING * q + RING):
            value = ptab[row : row + RS, j * LANES : (j + 1) * LANES] * (aux_ref[j : j + 1, :] - less)
            value = jnp.where(chosen == lane_of(j), value + gain, value)
            big = value.astype(jnp.bfloat16)
            gmat[q][j - RING * q, row : row + RS, :] = big
            glow[q][j - RING * q, row : row + RS, :] = (value - big.astype(jnp.float32)).astype(LOW)

    def pair_copy(k, first, count):
        rows = 12 * ROW_CHUNKS[k]
        src = cbuf.at[k % 2, pl.ds(first, count), pl.ds(pl.multiple_of((1 - core) * rows, 8), rows), :]
        return pltpu.make_async_remote_copy(
            src, drecv[k].at[pl.ds(first, count)], dsend.at[k], drsem.at[k], device_id=sibling, device_id_type=MESH)

    NT, KT = 256, 256

    def matmul_quarter(k, q, beside=()):
        rows = 24 * ROW_CHUNKS[k]
        base = 24 * offsets[k]
        if q == 0:
            if k >= 2:
                pair_copy(k - 2, 0, eblocks).wait_send()
        count = experts // RING // NT * 2 * (tok_rows // KT)
        beside = list(beside)
        each = -(-len(beside) // count)
        for n in range(experts // RING // NT):
            value = None
            for half in range(2):
                for kt in range(tok_rows // KT):
                    left, right = ((xt, gmat), (xlow, glow))[half]
                    right = [right[q][n * (NT // LANES) + j, kt * KT : (kt + 1) * KT, :] for j in range(NT // LANES)]
                    part = jnp.dot(
                        left[base : base + rows, kt * KT : (kt + 1) * KT], jnp.concatenate(right, axis=1), preferred_element_type=jnp.float32)
                    value = part if value is None else value + part
                    for piece in beside[:each]:
                        piece()
                    beside = beside[each:]
            for j in range(NT // LANES):
                cbuf[k % 2, RING * q + n * (NT // LANES) + j, 0:rows, :] = value[:, j * LANES : (j + 1) * LANES]
        pair_copy(k, RING * q, RING).start()

    orders = ("xyz", "yzx", "zxy")

    def pos(p, stage):
        return here[orders[p][stage]]

    def around(k, p, stage, numbers):
        axis, i = orders[p][stage], pos(p, stage)
        up, down, far = (i + 1) % RING, (i + 3) % RING, (i + 2) % RING
        right, left = away(axis, 1), away(axis, 3)
        s = (sums, tmid)[stage][k].at[p]
        m = (r1m, r2m)[stage][k].at[p]
        f = (r1f, r2f)[stage][k].at[p]
        table = (
            (s.at[far, 0:2], m.at[0], 0, right),
            (s.at[far, 2:4], m.at[1], 1, left),
            (s.at[up, 2:4], f.at[0, 2:4], 2, right),
            (s.at[down, 0:2], f.at[1, 0:2], 2, left),
            (s.at[up, 0:2], f.at[0, 0:2], 2, right),
            (s.at[down, 2:4], f.at[1, 2:4], 2, left),
            (s.at[up], f.at[0], 2, right),
            (s.at[down], f.at[1], 2, left),
        )
        copies = []
        for n in numbers:
            src, dst, sem, peer = table[n]
            copies.append(pltpu.make_async_remote_copy(src, dst, ssem.at[k, stage], rsem.at[k, p, 3 * stage + sem], device_id=peer, device_id_type=MESH))
        return copies

    def last_ring(k, p):
        axis, i = orders[p][2], pos(p, 2)
        return [
            pltpu.make_async_remote_copy(
                umid[k].at[p, (i + step) % RING], r3[k].at[p, step - 1], ssem.at[k, 2], rsem.at[k, p, 6], device_id=away(axis, step), device_id_type=MESH)
            for step in (1, 2, 3)
        ]

    def taken(ref, sem):
        pltpu.make_async_copy(ref, ref, sem).wait()

    def merge(k, p, stage):
        i = pos(p, stage)
        up, down = (i + 1) % RING, (i + 3) % RING
        s, m = (sums, tmid)[stage][k], (r1m, r2m)[stage][k]
        early = stage == 0 and k < EARLY_OWN
        first, second, third, fourth = around(k, p, stage, (0, 1, 4, 5) if early else (0, 1, 6, 7))
        first.wait_recv()
        s[p, up, 0:2] = s[p, up, 0:2] + m[p, 0]
        third.start()
        second.wait_recv()
        s[p, down, 2:4] = s[p, down, 2:4] + m[p, 1]
        fourth.start()

    def stage_a(k):
        pair_copy(k, 0, eblocks).wait_recv()
        r = ROW_CHUNKS[k]

        def block(e, carry):
            ye, xe = e // RING, e % RING
            for zz in range(RING):
                for p in range(3):
                    row = (zz * 3 + p) * r
                    mine = pl.ds(pl.multiple_of(core * (12 * r) + row, 8), r)
                    value = cbuf[k % 2, e, mine, :] + drecv[k][e, row : row + r, :]
                    at = {"x": xe, "y": ye, "z": zz}
                    sums[k][p, at[orders[p][0]], at[orders[p][1]], at[orders[p][2]]] = value
            return carry

        lax.fori_loop(0, eblocks, block, 0)
        for n in range(4 if k < EARLY_OWN else 2):
            for p in range(3):
                around(k, p, 0, (n,))[0].start()

    def stage_b(k):
        for p in range(3):
            merge(k, p, 0)

    def stage_c(k):
        for p in range(3):
            taken(r1f[k].at[p], rsem.at[k, p, 2])
            tmid[k][p] = sums[k][p, pos(p, 0)] + r1f[k][p, 0] + r1f[k][p, 1]
            for copy in around(k, p, 1, (0, 1)):
                copy.start()

    def stage_d(k):
        for p in range(3):
            merge(k, p, 1)

    def stage_e(k):
        for p in range(3):
            taken(r2f[k].at[p], rsem.at[k, p, 5])
            umid[k][p] = tmid[k][p, pos(p, 1)] + r2f[k][p, 0] + r2f[k][p, 1]
            for copy in last_ring(k, p):
                copy.start()
        taken(sums[k].at[:, 0:3], ssem.at[k, 0])

    def stage_f(k):
        r = ROW_CHUNKS[k]
        for p in range(3):
            taken(r3[k].at[p], rsem.at[k, p, 6])
            row = 88 * p + offsets[k]
            fin[row : row + r, :] = umid[k][p, pos(p, 2)] + r3[k][p, 0] + r3[k][p, 1] + r3[k][p, 2]
        taken(tmid[k].at[:, 0:3], ssem.at[k, 1])

    def plane_ring(k, p):
        (one, i), (two, j) = (orders[p][1], pos(p, 1)), (orders[p][2], pos(p, 2))
        copies = []
        for n in range(1, RING * RING):
            b, c = (i + n // RING) % RING, (j + n % RING) % RING
            copies.append(pltpu.make_async_remote_copy(
                tmid[k].at[p, b, c], plane[k].at[p, n - 1], ssem.at[k, 2], rsem.at[k, p, 6], device_id=device(**{one: b, two: c}), device_id_type=MESH))
        return copies

    def stage_plane(k):
        for p in range(3):
            taken(r1f[k].at[p], rsem.at[k, p, 2])
            tmid[k][p] = sums[k][p, pos(p, 0)] + r1f[k][p, 0] + r1f[k][p, 1]
            for copy in plane_ring(k, p):
                copy.start()
        taken(sums[k].at[:, 0:3], ssem.at[k, 0])

    def stage_g(k):
        r = ROW_CHUNKS[k]
        for p in range(3):
            taken(plane[k].at[p], rsem.at[k, p, 6])
            row = 88 * p + offsets[k]
            value = tmid[k][p, pos(p, 1), pos(p, 2)]
            for n in range(RING * RING - 1):
                value = value + plane[k][p, n]
            fin[row : row + r, :] = value

    def grad_pieces(q):
        return [functools.partial(grad_piece, q, row) for row in range(0, tok_rows, RS)]

    with jax.named_scope("first_chunk"):
        for piece in grad_pieces(0):
            piece()
        for q in range(RING):
            matmul_quarter(0, q, grad_pieces(q + 1) if q + 1 < RING else ())

    ring_stages = ((stage_a, 0.0), (stage_b, 0.088), (stage_c, 0.022), (stage_d, 0.044), (stage_e, 0.033), (stage_f, 0.0))
    plane_stages = ((stage_a, 0.0), (stage_b, 0.088), (stage_plane, 0.175), (stage_g, 0.0))
    quarters = [(k, q) for k in range(1, chunks) for q in range(RING)]
    ready = [(PAIR_TIME, 0, 0)]
    clock, links = 0.0, 0.0
    while quarters or ready:
        ready.sort()
        if ready and (ready[0][0] <= clock or not quarters):
            when, k, number = ready.pop(0)
            stages = plane_stages if k in PLANE else ring_stages
            stage, wire = stages[number]
            r = ROW_CHUNKS[k]
            clock = max(clock, when) + (0.04 if number else 0.025 * r)
            with jax.named_scope(f"{stage.__name__}_{k}"):
                stage(k)
            if number == 0:
                arrival = max(clock, links) + 0.088 * r
                links = arrival + (0.088 * r if k < EARLY_OWN else 0.0)
            else:
                arrival = links = max(clock, links) + wire * r * (1 if number > 1 or k < EARLY_OWN else 2)
            if number + 1 < len(stages):
                ready.append((arrival + HOP_TIME + (1.5 if stage is stage_plane else 0.0), k, number + 1))
        else:
            k, q = quarters.pop(0)
            with jax.named_scope(f"matmul_{k}"):
                matmul_quarter(k, q)
            clock += QUARTER_TIME * ROW_CHUNKS[k]
            if q == RING - 1:
                ready.append((clock + PAIR_TIME, k, 0))

    keep = keep_ref[pl.ds(ex, 1), :].astype(jnp.float32)
    rows = d_model // 8
    whole = fin[...] * (keep / scale)
    first, second = whole[0:rows, :], whole[whole.shape[0] - rows :, :]
    out_ref[...] = jnp.where(core == 0, first, second)

    taken(cnt_recv.at[0:7], csend.at[0])
    taken(cnt_recv.at[0:3], csend.at[1])
    taken(cnt_recv.at[0:3], csend.at[2])
    for k in range(max(chunks - 2, 0), chunks):
        pair_copy(k, 0, eblocks).wait_send()
    for k in range(chunks):
        taken(plane[k] if k in PLANE else umid[k].at[:, 0:3], ssem.at[k, 2])


def solution(mesh):
    devices = mesh.devices.size

    def local(tokens, router_logits, gate_grad, expert_index, keep_mask):
        tok_rows, d_model = tokens.shape
        experts = router_logits.shape[1]
        eblocks = experts // LANES
        chunks = len(ROW_CHUNKS)
        f32, bf16, i32 = jnp.float32, jnp.bfloat16, jnp.int32
        rmax = max(ROW_CHUNKS)
        vm = pltpu.VMEM

        def per_chunk(shape_of):
            return [vm(shape_of(r), f32) for r in ROW_CHUNKS]

        scratch = [
            vm((SLOTS, TB, experts), bf16),
            vm((tok_rows, LANES), i32),
            vm((tok_rows, LANES), f32),
            vm((tok_rows, LANES), f32),
            vm((tok_rows, experts), f32),
            [vm((RING, tok_rows, LANES), bf16)] * RING,
            [vm((RING, tok_rows, LANES), LOW)] * RING,
            vm((24 * sum(ROW_CHUNKS), tok_rows), bf16),
            vm((24 * sum(ROW_CHUNKS), tok_rows), LOW),
            vm((2, eblocks, 24 * rmax, LANES), f32),
            per_chunk(lambda r: (eblocks, 12 * r, LANES)),
            per_chunk(lambda r: (3, 4, 4, 4, r, LANES)),
            per_chunk(lambda r: (3, 2, 2, 4, r, LANES)),
            per_chunk(lambda r: (3, 2, 4, 4, r, LANES)),
            per_chunk(lambda r: (3, 4, 4, r, LANES)),
            per_chunk(lambda r: (3, 2, 2, r, LANES)),
            per_chunk(lambda r: (3, 2, 4, r, LANES)),
            per_chunk(lambda r: (3, 4, r, LANES)),
            per_chunk(lambda r: (3, 3, r, LANES)),
            [vm((3, RING * RING - 1, r if k in PLANE else 8, LANES), f32) for k, r in enumerate(ROW_CHUNKS)],
            vm((264, LANES), f32),
            vm((3, eblocks, LANES), i32),
            vm((13, eblocks, LANES), i32),
            vm((eblocks, LANES), f32),
            pltpu.SemaphoreType.DMA((SLOTS,)),
            pltpu.SemaphoreType.DMA((chunks,)),
            pltpu.SemaphoreType.DMA((3,)),
            pltpu.SemaphoreType.DMA((13,)),
            pltpu.SemaphoreType.DMA((chunks,)),
            pltpu.SemaphoreType.DMA((chunks,)),
            pltpu.SemaphoreType.DMA((chunks, 3)),
            pltpu.SemaphoreType.DMA((chunks, 3, 7)),
        ]
        return pl.pallas_call(
            functools.partial(kernel, tok_rows * devices),
            out_shape=jax.ShapeDtypeStruct((d_model // 8, LANES), f32),
            in_specs=[pl.BlockSpec(memory_space=pltpu.VMEM)] * 3 + [pl.BlockSpec(memory_space=pl.ANY)] * 2,
            out_specs=pl.BlockSpec(memory_space=pltpu.VMEM),
            scratch_shapes=scratch,
            compiler_params=pltpu.CompilerParams(collective_id=0, has_side_effects=True, vmem_limit_bytes=67043328),
        )(
            expert_index.reshape(tok_rows // LANES, LANES),
            gate_grad.reshape(tok_rows // LANES, LANES),
            keep_mask.reshape(eblocks, LANES),
            tokens.T,
            router_logits,
        ).T

    return jax.shard_map(
        local,
        mesh=mesh,
        in_specs=(P(("dp", "expert"), None), P(("dp", "expert"), None), P(("dp", "expert")), P(("dp", "expert"), None), P()),
        out_specs=P("expert", "dp"),
        check_vma=False,
    )
```

```python
import functools

import jax
import jax.numpy as jnp
from jax import lax
from jax.experimental import pallas as pl
from jax.experimental.pallas import tpu as pltpu
from jax.sharding import PartitionSpec as P

MESH = pl.DeviceIdType.MESH
RING = 4
LOW = jnp.float8_e5m2
PAIR_TIME, HOP_TIME, QUARTER_TIME = 1.1, 2.4, 0.046
PLANE = (6,)
EARLY_OWN = 6
LANES = 128
ROW_CHUNKS = (8, 16, 16, 16, 16, 8, 8)
TB = 128
SLOTS = 3


def kernel(total_tokens, idx_ref, gate_ref, keep_ref, tok_ref, logit_ref, out_ref,
           lbuf, icol, acol, drop, ptab, gmat, glow, xt, xlow, cbuf, drecv, sums, r1m, r1f, tmid, r2m, r2f, umid, r3, plane,
           fin, cnt, cnt_recv, aux_ref,
           lsem, xsem, csend, crecv, dsend, drsem, ssem, rsem):
    d_model, tok_rows = tok_ref.shape
    experts = logit_ref.shape[1]
    eblocks = experts // LANES
    blocks = tok_rows // TB
    chunks = len(ROW_CHUNKS)
    offsets = [sum(ROW_CHUNKS[:k]) for k in range(chunks)]

    dp = lax.axis_index("dp")
    ex = lax.axis_index("expert")
    zc, core = dp // 2, dp % 2
    yc, xc = ex // RING, ex % RING
    here = {"x": xc, "y": yc, "z": zc}

    def device(**moved):
        at = dict(here, **moved)
        return (2 * at["z"] + core, RING * at["y"] + at["x"])

    sibling = (2 * zc + 1 - core, ex)
    same_column = [((dp + step) % 8, ex) for step in range(1, 8)]

    def away(axis, step):
        return device(**{axis: (here[axis] + step) % RING})

    def load_logits(b, slot):
        return pltpu.make_async_copy(logit_ref.at[pl.ds(b * TB, TB), :], lbuf.at[slot], lsem.at[slot])

    for b in range(SLOTS):
        load_logits(b, b).start()

    barrier = pltpu.get_barrier_semaphore()
    peers = same_column + [away(axis, step) for axis in "xy" for step in (1, 2, 3)]
    for peer in peers:
        pl.semaphore_signal(barrier, inc=1, device_id=peer, device_id_type=MESH)

    idx = idx_ref[...]
    total = jnp.zeros((eblocks, LANES), jnp.float32)
    for b in range(blocks):
        row = idx[b : b + 1, :]
        high = (row // LANES == lax.broadcasted_iota(jnp.int32, (eblocks, LANES), 0)).astype(jnp.bfloat16)
        low = (row % LANES == lax.broadcasted_iota(jnp.int32, (LANES, LANES), 0)).astype(jnp.bfloat16)
        total = total + lax.dot_general(high, low, (((1,), (1,)), ((), ())), preferred_element_type=jnp.float32)
    cnt[0] = total.astype(jnp.int32)

    def count_copies(stage):
        targets = same_column if stage == 0 else [away("xy"[stage - 1], step) for step in (1, 2, 3)]
        first = (0, 7, 10)[stage]
        return [
            pltpu.make_async_remote_copy(cnt.at[stage], cnt_recv.at[first + n], csend.at[stage], crecv.at[first + n], device_id=target, device_id_type=MESH)
            for n, target in enumerate(targets)
        ]

    def count_arrive(stage):
        value = cnt[stage]
        for number, copy in enumerate(count_copies(stage)):
            copy.wait_recv()
            value = value + cnt_recv[(0, 7, 10)[stage] + number]
        return value

    def count_step(stage):
        cnt[stage + 1] = count_arrive(stage)
        for copy in count_copies(stage + 1):
            copy.start()

    idx_t = jnp.transpose(idx.astype(jnp.float32))
    gate_t = jnp.transpose(gate_ref[...])
    for b in range(blocks):
        icol[b * TB : (b + 1) * TB, :] = jnp.broadcast_to(idx_t[:, b : b + 1], (TB, LANES)).astype(jnp.int32)
        acol[b * TB : (b + 1) * TB, :] = jnp.broadcast_to(gate_t[:, b : b + 1], (TB, LANES))

    RS = 32

    def lane_of(j):
        return lax.broadcasted_iota(jnp.int32, (RS, LANES), 1) + j * LANES

    def stats_block(b):
        slot = b % SLOTS
        load_logits(b, slot).wait()

        def rows(r, carry):
            local = pl.ds(pl.multiple_of(r * RS, RS), RS)
            at = pl.ds(pl.multiple_of(b * TB + r * RS, RS), RS)
            peak = lbuf[slot, local, 0:LANES].astype(jnp.float32)
            for j in range(1, eblocks):
                peak = jnp.maximum(peak, lbuf[slot, local, j * LANES : (j + 1) * LANES].astype(jnp.float32))
            peak = jnp.max(peak, axis=1, keepdims=True)
            mass = jnp.zeros((RS, LANES), jnp.float32)
            top = jnp.zeros((RS, LANES), jnp.float32)
            chosen = icol[at, :]
            for j in range(eblocks):
                weight = jnp.exp(lbuf[slot, local, j * LANES : (j + 1) * LANES].astype(jnp.float32) - peak)
                ptab[at, j * LANES : (j + 1) * LANES] = weight
                mass = mass + weight
                top = top + jnp.where(chosen == lane_of(j), weight, 0.0)
            inverse = 1.0 / jnp.sum(mass, axis=1, keepdims=True)
            top_prob = jnp.sum(top, axis=1, keepdims=True) * inverse
            acol[at, :] = acol[at, :] * top_prob
            for j in range(eblocks):
                ptab[at, j * LANES : (j + 1) * LANES] = ptab[at, j * LANES : (j + 1) * LANES] * inverse
            return carry

        lax.fori_loop(0, TB // RS, rows, 0)

    def prep(b, carry):
        stats_block(b)

        @pl.when(b + SLOTS < blocks)
        def _():
            load_logits(b + SLOTS, b % SLOTS).start()

        return carry

    with jax.named_scope("prep_0"):
        lax.fori_loop(0, 2, prep, 0)
    with jax.named_scope("barrier"):
        pl.semaphore_wait(barrier, len(peers))
    for copy in count_copies(0):
        copy.start()

    for k in range(chunks):
        r = ROW_CHUNKS[k]
        for group in range(24):
            cc, zz, part = group // 12, (group // 3) % 4, group % 3
            src = (d_model // RING) * zz + 256 * cc + 88 * part + offsets[k]
            dst = 24 * offsets[k] + r * group
            pltpu.make_async_copy(tok_ref.at[pl.ds(src, r), :], xt.at[pl.ds(dst, r), :], xsem.at[k]).start()

    with jax.named_scope("prep_1"):
        lax.fori_loop(2, 5, prep, 0)
    with jax.named_scope("count_step_0"):
        count_step(0)
    with jax.named_scope("prep_2"):
        lax.fori_loop(5, 8, prep, 0)
    with jax.named_scope("count_step_1"):
        count_step(1)
    def lower_rows(n, carry):
        at = pl.ds(pl.multiple_of(n * LR, LR), LR)
        xlow[at, :] = xt[at, :].astype(LOW)
        return carry

    LR = 96
    with jax.named_scope("lower"):
        for k in range(chunks):
            chunk_rows = xt.at[pl.ds(24 * offsets[k], 24 * ROW_CHUNKS[k]), :]
            pltpu.make_async_copy(chunk_rows, chunk_rows, xsem.at[k]).wait()
        lax.fori_loop(0, 24 * sum(ROW_CHUNKS) // LR, lower_rows, 0)

    with jax.named_scope("count_last"):
        raw = count_arrive(2).astype(jnp.float32) * (experts / total_tokens)
        scale = 4194304.0 / (jnp.max(jnp.max(raw, axis=1, keepdims=True), axis=0, keepdims=True) + 6.0)
        aux_ref[...] = raw * scale

    def spread_rows(r, carry):
        at = pl.ds(pl.multiple_of(r * RS, RS), RS)
        acc = ptab[at, 0:LANES] * aux_ref[0:1, :]
        for j in range(1, eblocks):
            acc = acc + ptab[at, j * LANES : (j + 1) * LANES] * aux_ref[j : j + 1, :]
        gain = acol[at, :] * scale
        acol[at, :] = gain
        drop[at, :] = jnp.sum(acc, axis=1, keepdims=True) + gain
        return carry

    with jax.named_scope("spread"):
        lax.fori_loop(0, tok_rows // RS, spread_rows, 0, unroll=8)

    def grad_piece(q, row):
        gain = acol[row : row + RS, :]
        less = drop[row : row + RS, :]
        chosen = icol[row : row + RS, :]
        for j in range(RING * q, RING * q + RING):
            value = ptab[row : row + RS, j * LANES : (j + 1) * LANES] * (aux_ref[j : j + 1, :] - less)
            value = jnp.where(chosen == lane_of(j), value + gain, value)
            big = value.astype(jnp.bfloat16)
            gmat[q][j - RING * q, row : row + RS, :] = big
            glow[q][j - RING * q, row : row + RS, :] = (value - big.astype(jnp.float32)).astype(LOW)

    def pair_copy(k, first, count):
        rows = 12 * ROW_CHUNKS[k]
        src = cbuf.at[k % 2, pl.ds(first, count), pl.ds(pl.multiple_of((1 - core) * rows, 8), rows), :]
        return pltpu.make_async_remote_copy(
            src, drecv[k].at[pl.ds(first, count)], dsend.at[k], drsem.at[k], device_id=sibling, device_id_type=MESH)

    NT, KT = 256, 256

    def matmul_quarter(k, q, beside=()):
        rows = 24 * ROW_CHUNKS[k]
        base = 24 * offsets[k]
        if q == 0:
            if k >= 2:
                pair_copy(k - 2, 0, eblocks).wait_send()
        count = experts // RING // NT * 2 * (tok_rows // KT)
        beside = list(beside)
        each = -(-len(beside) // count)
        for n in range(experts // RING // NT):
            value = None
            for half in range(2):
                for kt in range(tok_rows // KT):
                    left, right = ((xt, gmat), (xlow, glow))[half]
                    right = [right[q][n * (NT // LANES) + j, kt * KT : (kt + 1) * KT, :] for j in range(NT // LANES)]
                    part = jnp.dot(
                        left[base : base + rows, kt * KT : (kt + 1) * KT], jnp.concatenate(right, axis=1), preferred_element_type=jnp.float32)
                    value = part if value is None else value + part
                    for piece in beside[:each]:
                        piece()
                    beside = beside[each:]
            for j in range(NT // LANES):
                cbuf[k % 2, RING * q + n * (NT // LANES) + j, 0:rows, :] = value[:, j * LANES : (j + 1) * LANES]
        pair_copy(k, RING * q, RING).start()

    orders = ("xyz", "yzx", "zxy")

    def pos(p, stage):
        return here[orders[p][stage]]

    def around(k, p, stage, numbers):
        axis, i = orders[p][stage], pos(p, stage)
        up, down, far = (i + 1) % RING, (i + 3) % RING, (i + 2) % RING
        right, left = away(axis, 1), away(axis, 3)
        s = (sums, tmid)[stage][k].at[p]
        m = (r1m, r2m)[stage][k].at[p]
        f = (r1f, r2f)[stage][k].at[p]
        table = (
            (s.at[far, 0:2], m.at[0], 0, right),
            (s.at[far, 2:4], m.at[1], 1, left),
            (s.at[up, 2:4], f.at[0, 2:4], 2, right),
            (s.at[down, 0:2], f.at[1, 0:2], 2, left),
            (s.at[up, 0:2], f.at[0, 0:2], 2, right),
            (s.at[down, 2:4], f.at[1, 2:4], 2, left),
            (s.at[up], f.at[0], 2, right),
            (s.at[down], f.at[1], 2, left),
        )
        copies = []
        for n in numbers:
            src, dst, sem, peer = table[n]
            copies.append(pltpu.make_async_remote_copy(src, dst, ssem.at[k, stage], rsem.at[k, p, 3 * stage + sem], device_id=peer, device_id_type=MESH))
        return copies

    def last_ring(k, p):
        axis, i = orders[p][2], pos(p, 2)
        return [
            pltpu.make_async_remote_copy(
                umid[k].at[p, (i + step) % RING], r3[k].at[p, step - 1], ssem.at[k, 2], rsem.at[k, p, 6], device_id=away(axis, step), device_id_type=MESH)
            for step in (1, 2, 3)
        ]

    def taken(ref, sem):
        pltpu.make_async_copy(ref, ref, sem).wait()

    def merge(k, p, stage):
        i = pos(p, stage)
        up, down = (i + 1) % RING, (i + 3) % RING
        s, m = (sums, tmid)[stage][k], (r1m, r2m)[stage][k]
        early = stage == 0 and k < EARLY_OWN
        first, second, third, fourth = around(k, p, stage, (0, 1, 4, 5) if early else (0, 1, 6, 7))
        first.wait_recv()
        s[p, up, 0:2] = s[p, up, 0:2] + m[p, 0]
        third.start()
        second.wait_recv()
        s[p, down, 2:4] = s[p, down, 2:4] + m[p, 1]
        fourth.start()

    def stage_a(k):
        pair_copy(k, 0, eblocks).wait_recv()
        r = ROW_CHUNKS[k]

        def block(e, carry):
            ye, xe = e // RING, e % RING
            for zz in range(RING):
                for p in range(3):
                    row = (zz * 3 + p) * r
                    mine = pl.ds(pl.multiple_of(core * (12 * r) + row, 8), r)
                    value = cbuf[k % 2, e, mine, :] + drecv[k][e, row : row + r, :]
                    at = {"x": xe, "y": ye, "z": zz}
                    sums[k][p, at[orders[p][0]], at[orders[p][1]], at[orders[p][2]]] = value
            return carry

        lax.fori_loop(0, eblocks, block, 0)
        for n in range(4 if k < EARLY_OWN else 2):
            for p in range(3):
                around(k, p, 0, (n,))[0].start()

    def stage_b(k):
        for p in range(3):
            merge(k, p, 0)

    def stage_c(k):
        for p in range(3):
            taken(r1f[k].at[p], rsem.at[k, p, 2])
            tmid[k][p] = sums[k][p, pos(p, 0)] + r1f[k][p, 0] + r1f[k][p, 1]
            for copy in around(k, p, 1, (0, 1)):
                copy.start()

    def stage_d(k):
        for p in range(3):
            merge(k, p, 1)

    def stage_e(k):
        for p in range(3):
            taken(r2f[k].at[p], rsem.at[k, p, 5])
            umid[k][p] = tmid[k][p, pos(p, 1)] + r2f[k][p, 0] + r2f[k][p, 1]
            for copy in last_ring(k, p):
                copy.start()
        taken(sums[k].at[:, 0:3], ssem.at[k, 0])

    def stage_f(k):
        r = ROW_CHUNKS[k]
        for p in range(3):
            taken(r3[k].at[p], rsem.at[k, p, 6])
            row = 88 * p + offsets[k]
            fin[row : row + r, :] = umid[k][p, pos(p, 2)] + r3[k][p, 0] + r3[k][p, 1] + r3[k][p, 2]
        taken(tmid[k].at[:, 0:3], ssem.at[k, 1])

    def plane_ring(k, p):
        (one, i), (two, j) = (orders[p][1], pos(p, 1)), (orders[p][2], pos(p, 2))
        copies = []
        for n in range(1, RING * RING):
            b, c = (i + n // RING) % RING, (j + n % RING) % RING
            copies.append(pltpu.make_async_remote_copy(
                tmid[k].at[p, b, c], plane[k].at[p, n - 1], ssem.at[k, 2], rsem.at[k, p, 6], device_id=device(**{one: b, two: c}), device_id_type=MESH))
        return copies

    def stage_plane(k):
        for p in range(3):
            taken(r1f[k].at[p], rsem.at[k, p, 2])
            tmid[k][p] = sums[k][p, pos(p, 0)] + r1f[k][p, 0] + r1f[k][p, 1]
            for copy in plane_ring(k, p):
                copy.start()
        taken(sums[k].at[:, 0:3], ssem.at[k, 0])

    def stage_g(k):
        r = ROW_CHUNKS[k]
        for p in range(3):
            taken(plane[k].at[p], rsem.at[k, p, 6])
            row = 88 * p + offsets[k]
            value = tmid[k][p, pos(p, 1), pos(p, 2)]
            for n in range(RING * RING - 1):
                value = value + plane[k][p, n]
            fin[row : row + r, :] = value

    def grad_pieces(q):
        return [functools.partial(grad_piece, q, row) for row in range(0, tok_rows, RS)]

    with jax.named_scope("first_chunk"):
        for piece in grad_pieces(0):
            piece()
        for q in range(RING):
            matmul_quarter(0, q, grad_pieces(q + 1) if q + 1 < RING else ())

    ring_stages = ((stage_a, 0.0), (stage_b, 0.088), (stage_c, 0.022), (stage_d, 0.044), (stage_e, 0.033), (stage_f, 0.0))
    plane_stages = ((stage_a, 0.0), (stage_b, 0.088), (stage_plane, 0.175), (stage_g, 0.0))
    quarters = [(k, q) for k in range(1, chunks) for q in range(RING)]
    ready = [(PAIR_TIME, 0, 0)]
    clock, links = 0.0, 0.0
    while quarters or ready:
        ready.sort()
        if ready and (ready[0][0] <= clock or not quarters):
            when, k, number = ready.pop(0)
            stages = plane_stages if k in PLANE else ring_stages
            stage, wire = stages[number]
            r = ROW_CHUNKS[k]
            clock = max(clock, when) + (0.04 if number else 0.025 * r)
            with jax.named_scope(f"{stage.__name__}_{k}"):
                stage(k)
            if number == 0:
                arrival = max(clock, links) + 0.088 * r
                links = arrival + (0.088 * r if k < EARLY_OWN else 0.0)
            else:
                arrival = links = max(clock, links) + wire * r * (1 if number > 1 or k < EARLY_OWN else 2)
            if number + 1 < len(stages):
                ready.append((arrival + HOP_TIME + (1.5 if stage is stage_plane else 0.0), k, number + 1))
        else:
            k, q = quarters.pop(0)
            with jax.named_scope(f"matmul_{k}"):
                matmul_quarter(k, q)
            clock += QUARTER_TIME * ROW_CHUNKS[k]
            if q == RING - 1:
                ready.append((clock + PAIR_TIME, k, 0))

    keep = keep_ref[pl.ds(ex, 1), :].astype(jnp.float32)
    rows = d_model // 8
    whole = fin[...] * (keep / scale)
    first, second = whole[0:rows, :], whole[whole.shape[0] - rows :, :]
    out_ref[...] = jnp.where(core == 0, first, second)

    taken(cnt_recv.at[0:7], csend.at[0])
    taken(cnt_recv.at[0:3], csend.at[1])
    taken(cnt_recv.at[0:3], csend.at[2])
    for k in range(max(chunks - 2, 0), chunks):
        pair_copy(k, 0, eblocks).wait_send()
    for k in range(chunks):
        taken(plane[k] if k in PLANE else umid[k].at[:, 0:3], ssem.at[k, 2])


def solution(mesh):
    devices = mesh.devices.size

    def local(tokens, router_logits, gate_grad, expert_index, keep_mask):
        tok_rows, d_model = tokens.shape
        experts = router_logits.shape[1]
        eblocks = experts // LANES
        chunks = len(ROW_CHUNKS)
        f32, bf16, i32 = jnp.float32, jnp.bfloat16, jnp.int32
        rmax = max(ROW_CHUNKS)
        vm = pltpu.VMEM

        def per_chunk(shape_of):
            return [vm(shape_of(r), f32) for r in ROW_CHUNKS]

        scratch = [
            vm((SLOTS, TB, experts), bf16),
            vm((tok_rows, LANES), i32),
            vm((tok_rows, LANES), f32),
            vm((tok_rows, LANES), f32),
            vm((tok_rows, experts), f32),
            [vm((RING, tok_rows, LANES), bf16)] * RING,
            [vm((RING, tok_rows, LANES), LOW)] * RING,
            vm((24 * sum(ROW_CHUNKS), tok_rows), bf16),
            vm((24 * sum(ROW_CHUNKS), tok_rows), LOW),
            vm((2, eblocks, 24 * rmax, LANES), f32),
            per_chunk(lambda r: (eblocks, 12 * r, LANES)),
            per_chunk(lambda r: (3, 4, 4, 4, r, LANES)),
            per_chunk(lambda r: (3, 2, 2, 4, r, LANES)),
            per_chunk(lambda r: (3, 2, 4, 4, r, LANES)),
            per_chunk(lambda r: (3, 4, 4, r, LANES)),
            per_chunk(lambda r: (3, 2, 2, r, LANES)),
            per_chunk(lambda r: (3, 2, 4, r, LANES)),
            per_chunk(lambda r: (3, 4, r, LANES)),
            per_chunk(lambda r: (3, 3, r, LANES)),
            [vm((3, RING * RING - 1, r if k in PLANE else 8, LANES), f32) for k, r in enumerate(ROW_CHUNKS)],
            vm((264, LANES), f32),
            vm((3, eblocks, LANES), i32),
            vm((13, eblocks, LANES), i32),
            vm((eblocks, LANES), f32),
            pltpu.SemaphoreType.DMA((SLOTS,)),
            pltpu.SemaphoreType.DMA((chunks,)),
            pltpu.SemaphoreType.DMA((3,)),
            pltpu.SemaphoreType.DMA((13,)),
            pltpu.SemaphoreType.DMA((chunks,)),
            pltpu.SemaphoreType.DMA((chunks,)),
            pltpu.SemaphoreType.DMA((chunks, 3)),
            pltpu.SemaphoreType.DMA((chunks, 3, 7)),
        ]
        return pl.pallas_call(
            functools.partial(kernel, tok_rows * devices),
            out_shape=jax.ShapeDtypeStruct((d_model // 8, LANES), f32),
            in_specs=[pl.BlockSpec(memory_space=pltpu.VMEM)] * 3 + [pl.BlockSpec(memory_space=pl.ANY)] * 2,
            out_specs=pl.BlockSpec(memory_space=pltpu.VMEM),
            scratch_shapes=scratch,
            compiler_params=pltpu.CompilerParams(collective_id=0, has_side_effects=True, vmem_limit_bytes=67043328),
        )(
            expert_index.reshape(tok_rows // LANES, LANES),
            gate_grad.reshape(tok_rows // LANES, LANES),
            keep_mask.reshape(eblocks, LANES),
            tokens.T,
            router_logits,
        ).T

    return jax.shard_map(
        local,
        mesh=mesh,
        in_specs=(P(("dp", "expert"), None), P(("dp", "expert"), None), P(("dp", "expert")), P(("dp", "expert"), None), P()),
        out_specs=P("expert", "dp"),
        check_vma=False,
    )
```

```python
import functools

import jax
import jax.numpy as jnp
from jax import lax
from jax.experimental import pallas as pl
from jax.experimental.pallas import tpu as pltpu
from jax.sharding import PartitionSpec as P

MESH = pl.DeviceIdType.MESH
RING = 4
LOW = jnp.float8_e5m2
PAIR_TIME, HOP_TIME, QUARTER_TIME = 1.1, 2.4, 0.046
PLANE = (6,)
EARLY_OWN = 6
LANES = 128
ROW_CHUNKS = (8, 16, 16, 16, 16, 8, 8)
TB = 128
SLOTS = 3


def kernel(total_tokens, idx_ref, gate_ref, keep_ref, tok_ref, logit_ref, out_ref,
           lbuf, icol, acol, drop, ptab, gmat, glow, xt, xlow, cbuf, drecv, sums, r1m, r1f, tmid, r2m, r2f, umid, r3, plane,
           fin, cnt, cnt_recv, aux_ref,
           lsem, xsem, csend, crecv, dsend, drsem, ssem, rsem):
    d_model, tok_rows = tok_ref.shape
    experts = logit_ref.shape[1]
    eblocks = experts // LANES
    blocks = tok_rows // TB
    chunks = len(ROW_CHUNKS)
    offsets = [sum(ROW_CHUNKS[:k]) for k in range(chunks)]

    dp = lax.axis_index("dp")
    ex = lax.axis_index("expert")
    zc, core = dp // 2, dp % 2
    yc, xc = ex // RING, ex % RING
    here = {"x": xc, "y": yc, "z": zc}

    def device(**moved):
        at = dict(here, **moved)
        return (2 * at["z"] + core, RING * at["y"] + at["x"])

    sibling = (2 * zc + 1 - core, ex)
    same_column = [((dp + step) % 8, ex) for step in range(1, 8)]

    def away(axis, step):
        return device(**{axis: (here[axis] + step) % RING})

    def load_logits(b, slot):
        return pltpu.make_async_copy(logit_ref.at[pl.ds(b * TB, TB), :], lbuf.at[slot], lsem.at[slot])

    for b in range(SLOTS):
        load_logits(b, b).start()

    barrier = pltpu.get_barrier_semaphore()
    peers = same_column + [away(axis, step) for axis in "xy" for step in (1, 2, 3)]
    for peer in peers:
        pl.semaphore_signal(barrier, inc=1, device_id=peer, device_id_type=MESH)

    idx = idx_ref[...]
    total = jnp.zeros((eblocks, LANES), jnp.float32)
    for b in range(blocks):
        row = idx[b : b + 1, :]
        high = (row // LANES == lax.broadcasted_iota(jnp.int32, (eblocks, LANES), 0)).astype(jnp.bfloat16)
        low = (row % LANES == lax.broadcasted_iota(jnp.int32, (LANES, LANES), 0)).astype(jnp.bfloat16)
        total = total + lax.dot_general(high, low, (((1,), (1,)), ((), ())), preferred_element_type=jnp.float32)
    cnt[0] = total.astype(jnp.int32)

    def count_copies(stage):
        targets = same_column if stage == 0 else [away("xy"[stage - 1], step) for step in (1, 2, 3)]
        first = (0, 7, 10)[stage]
        return [
            pltpu.make_async_remote_copy(cnt.at[stage], cnt_recv.at[first + n], csend.at[stage], crecv.at[first + n], device_id=target, device_id_type=MESH)
            for n, target in enumerate(targets)
        ]

    def count_arrive(stage):
        value = cnt[stage]
        for number, copy in enumerate(count_copies(stage)):
            copy.wait_recv()
            value = value + cnt_recv[(0, 7, 10)[stage] + number]
        return value

    def count_step(stage):
        cnt[stage + 1] = count_arrive(stage)
        for copy in count_copies(stage + 1):
            copy.start()

    idx_t = jnp.transpose(idx.astype(jnp.float32))
    gate_t = jnp.transpose(gate_ref[...])
    for b in range(blocks):
        icol[b * TB : (b + 1) * TB, :] = jnp.broadcast_to(idx_t[:, b : b + 1], (TB, LANES)).astype(jnp.int32)
        acol[b * TB : (b + 1) * TB, :] = jnp.broadcast_to(gate_t[:, b : b + 1], (TB, LANES))

    RS = 32

    def lane_of(j):
        return lax.broadcasted_iota(jnp.int32, (RS, LANES), 1) + j * LANES

    def stats_block(b):
        slot = b % SLOTS
        load_logits(b, slot).wait()

        def rows(r, carry):
            local = pl.ds(pl.multiple_of(r * RS, RS), RS)
            at = pl.ds(pl.multiple_of(b * TB + r * RS, RS), RS)
            peak = lbuf[slot, local, 0:LANES].astype(jnp.float32)
            for j in range(1, eblocks):
                peak = jnp.maximum(peak, lbuf[slot, local, j * LANES : (j + 1) * LANES].astype(jnp.float32))
            peak = jnp.max(peak, axis=1, keepdims=True)
            mass = jnp.zeros((RS, LANES), jnp.float32)
            top = jnp.zeros((RS, LANES), jnp.float32)
            chosen = icol[at, :]
            for j in range(eblocks):
                weight = jnp.exp(lbuf[slot, local, j * LANES : (j + 1) * LANES].astype(jnp.float32) - peak)
                ptab[at, j * LANES : (j + 1) * LANES] = weight
                mass = mass + weight
                top = top + jnp.where(chosen == lane_of(j), weight, 0.0)
            inverse = 1.0 / jnp.sum(mass, axis=1, keepdims=True)
            top_prob = jnp.sum(top, axis=1, keepdims=True) * inverse
            acol[at, :] = acol[at, :] * top_prob
            for j in range(eblocks):
                ptab[at, j * LANES : (j + 1) * LANES] = ptab[at, j * LANES : (j + 1) * LANES] * inverse
            return carry

        lax.fori_loop(0, TB // RS, rows, 0)

    def prep(b, carry):
        stats_block(b)

        @pl.when(b + SLOTS < blocks)
        def _():
            load_logits(b + SLOTS, b % SLOTS).start()

        return carry

    with jax.named_scope("prep_0"):
        lax.fori_loop(0, 2, prep, 0)
    with jax.named_scope("barrier"):
        pl.semaphore_wait(barrier, len(peers))
    for copy in count_copies(0):
        copy.start()

    for k in range(chunks):
        r = ROW_CHUNKS[k]
        for group in range(24):
            cc, zz, part = group // 12, (group // 3) % 4, group % 3
            src = (d_model // RING) * zz + 256 * cc + 88 * part + offsets[k]
            dst = 24 * offsets[k] + r * group
            pltpu.make_async_copy(tok_ref.at[pl.ds(src, r), :], xt.at[pl.ds(dst, r), :], xsem.at[k]).start()

    with jax.named_scope("prep_1"):
        lax.fori_loop(2, 5, prep, 0)
    with jax.named_scope("count_step_0"):
        count_step(0)
    with jax.named_scope("prep_2"):
        lax.fori_loop(5, 7, prep, 0)
    with jax.named_scope("count_step_1"):
        count_step(1)
    with jax.named_scope("prep_3"):
        lax.fori_loop(7, 8, prep, 0)
    def lower_rows(n, carry):
        at = pl.ds(pl.multiple_of(n * LR, LR), LR)
        xlow[at, :] = xt[at, :].astype(LOW)
        return carry

    LR = 96
    with jax.named_scope("lower"):
        for k in range(chunks):
            chunk_rows = xt.at[pl.ds(24 * offsets[k], 24 * ROW_CHUNKS[k]), :]
            pltpu.make_async_copy(chunk_rows, chunk_rows, xsem.at[k]).wait()
        lax.fori_loop(0, 24 * sum(ROW_CHUNKS) // LR, lower_rows, 0)

    with jax.named_scope("count_last"):
        raw = count_arrive(2).astype(jnp.float32) * (experts / total_tokens)
        scale = 4194304.0 / (jnp.max(jnp.max(raw, axis=1, keepdims=True), axis=0, keepdims=True) + 6.0)
        aux_ref[...] = raw * scale

    def spread_rows(r, carry):
        at = pl.ds(pl.multiple_of(r * RS, RS), RS)
        acc = ptab[at, 0:LANES] * aux_ref[0:1, :]
        for j in range(1, eblocks):
            acc = acc + ptab[at, j * LANES : (j + 1) * LANES] * aux_ref[j : j + 1, :]
        gain = acol[at, :] * scale
        acol[at, :] = gain
        drop[at, :] = jnp.sum(acc, axis=1, keepdims=True) + gain
        return carry

    with jax.named_scope("spread"):
        lax.fori_loop(0, tok_rows // RS, spread_rows, 0, unroll=8)

    def grad_piece(q, row):
        gain = acol[row : row + RS, :]
        less = drop[row : row + RS, :]
        chosen = icol[row : row + RS, :]
        for j in range(RING * q, RING * q + RING):
            value = ptab[row : row + RS, j * LANES : (j + 1) * LANES] * (aux_ref[j : j + 1, :] - less)
            value = jnp.where(chosen == lane_of(j), value + gain, value)
            big = value.astype(jnp.bfloat16)
            gmat[q][j - RING * q, row : row + RS, :] = big
            glow[q][j - RING * q, row : row + RS, :] = (value - big.astype(jnp.float32)).astype(LOW)

    def pair_copy(k, first, count):
        rows = 12 * ROW_CHUNKS[k]
        src = cbuf.at[k % 2, pl.ds(first, count), pl.ds(pl.multiple_of((1 - core) * rows, 8), rows), :]
        return pltpu.make_async_remote_copy(
            src, drecv[k].at[pl.ds(first, count)], dsend.at[k], drsem.at[k], device_id=sibling, device_id_type=MESH)

    NT, KT = 256, 256

    def matmul_quarter(k, q, beside=()):
        rows = 24 * ROW_CHUNKS[k]
        base = 24 * offsets[k]
        if q == 0:
            if k >= 2:
                pair_copy(k - 2, 0, eblocks).wait_send()
        count = experts // RING // NT * 2 * (tok_rows // KT)
        beside = list(beside)
        each = -(-len(beside) // count)
        for n in range(experts // RING // NT):
            value = None
            for half in range(2):
                for kt in range(tok_rows // KT):
                    left, right = ((xt, gmat), (xlow, glow))[half]
                    right = [right[q][n * (NT // LANES) + j, kt * KT : (kt + 1) * KT, :] for j in range(NT // LANES)]
                    part = jnp.dot(
                        left[base : base + rows, kt * KT : (kt + 1) * KT], jnp.concatenate(right, axis=1), preferred_element_type=jnp.float32)
                    value = part if value is None else value + part
                    for piece in beside[:each]:
                        piece()
                    beside = beside[each:]
            for j in range(NT // LANES):
                cbuf[k % 2, RING * q + n * (NT // LANES) + j, 0:rows, :] = value[:, j * LANES : (j + 1) * LANES]
        pair_copy(k, RING * q, RING).start()

    orders = ("xyz", "yzx", "zxy")

    def pos(p, stage):
        return here[orders[p][stage]]

    def around(k, p, stage, numbers):
        axis, i = orders[p][stage], pos(p, stage)
        up, down, far = (i + 1) % RING, (i + 3) % RING, (i + 2) % RING
        right, left = away(axis, 1), away(axis, 3)
        s = (sums, tmid)[stage][k].at[p]
        m = (r1m, r2m)[stage][k].at[p]
        f = (r1f, r2f)[stage][k].at[p]
        table = (
            (s.at[far, 0:2], m.at[0], 0, right),
            (s.at[far, 2:4], m.at[1], 1, left),
            (s.at[up, 2:4], f.at[0, 2:4], 2, right),
            (s.at[down, 0:2], f.at[1, 0:2], 2, left),
            (s.at[up, 0:2], f.at[0, 0:2], 2, right),
            (s.at[down, 2:4], f.at[1, 2:4], 2, left),
            (s.at[up], f.at[0], 2, right),
            (s.at[down], f.at[1], 2, left),
        )
        copies = []
        for n in numbers:
            src, dst, sem, peer = table[n]
            copies.append(pltpu.make_async_remote_copy(src, dst, ssem.at[k, stage], rsem.at[k, p, 3 * stage + sem], device_id=peer, device_id_type=MESH))
        return copies

    def last_ring(k, p):
        axis, i = orders[p][2], pos(p, 2)
        return [
            pltpu.make_async_remote_copy(
                umid[k].at[p, (i + step) % RING], r3[k].at[p, step - 1], ssem.at[k, 2], rsem.at[k, p, 6], device_id=away(axis, step), device_id_type=MESH)
            for step in (1, 2, 3)
        ]

    def taken(ref, sem):
        pltpu.make_async_copy(ref, ref, sem).wait()

    def merge(k, p, stage):
        i = pos(p, stage)
        up, down = (i + 1) % RING, (i + 3) % RING
        s, m = (sums, tmid)[stage][k], (r1m, r2m)[stage][k]
        early = stage == 0 and k < EARLY_OWN
        first, second, third, fourth = around(k, p, stage, (0, 1, 4, 5) if early else (0, 1, 6, 7))
        first.wait_recv()
        s[p, up, 0:2] = s[p, up, 0:2] + m[p, 0]
        third.start()
        second.wait_recv()
        s[p, down, 2:4] = s[p, down, 2:4] + m[p, 1]
        fourth.start()

    def stage_a(k):
        pair_copy(k, 0, eblocks).wait_recv()
        r = ROW_CHUNKS[k]

        def block(e, carry):
            ye, xe = e // RING, e % RING
            for zz in range(RING):
                for p in range(3):
                    row = (zz * 3 + p) * r
                    mine = pl.ds(pl.multiple_of(core * (12 * r) + row, 8), r)
                    value = cbuf[k % 2, e, mine, :] + drecv[k][e, row : row + r, :]
                    at = {"x": xe, "y": ye, "z": zz}
                    sums[k][p, at[orders[p][0]], at[orders[p][1]], at[orders[p][2]]] = value
            return carry

        lax.fori_loop(0, eblocks, block, 0)
        for n in range(4 if k < EARLY_OWN else 2):
            for p in range(3):
                around(k, p, 0, (n,))[0].start()

    def stage_b(k):
        for p in range(3):
            merge(k, p, 0)

    def stage_c(k):
        for p in range(3):
            taken(r1f[k].at[p], rsem.at[k, p, 2])
            tmid[k][p] = sums[k][p, pos(p, 0)] + r1f[k][p, 0] + r1f[k][p, 1]
            for copy in around(k, p, 1, (0, 1)):
                copy.start()

    def stage_d(k):
        for p in range(3):
            merge(k, p, 1)

    def stage_e(k):
        for p in range(3):
            taken(r2f[k].at[p], rsem.at[k, p, 5])
            umid[k][p] = tmid[k][p, pos(p, 1)] + r2f[k][p, 0] + r2f[k][p, 1]
            for copy in last_ring(k, p):
                copy.start()
        taken(sums[k].at[:, 0:3], ssem.at[k, 0])

    def stage_f(k):
        r = ROW_CHUNKS[k]
        for p in range(3):
            taken(r3[k].at[p], rsem.at[k, p, 6])
            row = 88 * p + offsets[k]
            fin[row : row + r, :] = umid[k][p, pos(p, 2)] + r3[k][p, 0] + r3[k][p, 1] + r3[k][p, 2]
        taken(tmid[k].at[:, 0:3], ssem.at[k, 1])

    def plane_ring(k, p):
        (one, i), (two, j) = (orders[p][1], pos(p, 1)), (orders[p][2], pos(p, 2))
        copies = []
        for n in range(1, RING * RING):
            b, c = (i + n // RING) % RING, (j + n % RING) % RING
            copies.append(pltpu.make_async_remote_copy(
                tmid[k].at[p, b, c], plane[k].at[p, n - 1], ssem.at[k, 2], rsem.at[k, p, 6], device_id=device(**{one: b, two: c}), device_id_type=MESH))
        return copies

    def stage_plane(k):
        for p in range(3):
            taken(r1f[k].at[p], rsem.at[k, p, 2])
            tmid[k][p] = sums[k][p, pos(p, 0)] + r1f[k][p, 0] + r1f[k][p, 1]
            for copy in plane_ring(k, p):
                copy.start()
        taken(sums[k].at[:, 0:3], ssem.at[k, 0])

    def stage_g(k):
        r = ROW_CHUNKS[k]
        for p in range(3):
            taken(plane[k].at[p], rsem.at[k, p, 6])
            row = 88 * p + offsets[k]
            value = tmid[k][p, pos(p, 1), pos(p, 2)]
            for n in range(RING * RING - 1):
                value = value + plane[k][p, n]
            fin[row : row + r, :] = value

    def grad_pieces(q):
        return [functools.partial(grad_piece, q, row) for row in range(0, tok_rows, RS)]

    with jax.named_scope("first_chunk"):
        for piece in grad_pieces(0):
            piece()
        for q in range(RING):
            matmul_quarter(0, q, grad_pieces(q + 1) if q + 1 < RING else ())

    ring_stages = ((stage_a, 0.0), (stage_b, 0.088), (stage_c, 0.022), (stage_d, 0.044), (stage_e, 0.033), (stage_f, 0.0))
    plane_stages = ((stage_a, 0.0), (stage_b, 0.088), (stage_plane, 0.175), (stage_g, 0.0))
    quarters = [(k, q) for k in range(1, chunks) for q in range(RING)]
    ready = [(PAIR_TIME, 0, 0)]
    clock, links = 0.0, 0.0
    while quarters or ready:
        ready.sort()
        if ready and (ready[0][0] <= clock or not quarters):
            when, k, number = ready.pop(0)
            stages = plane_stages if k in PLANE else ring_stages
            stage, wire = stages[number]
            r = ROW_CHUNKS[k]
            clock = max(clock, when) + (0.04 if number else 0.025 * r)
            with jax.named_scope(f"{stage.__name__}_{k}"):
                stage(k)
            if number == 0:
                arrival = max(clock, links) + 0.088 * r
                links = arrival + (0.088 * r if k < EARLY_OWN else 0.0)
            else:
                arrival = links = max(clock, links) + wire * r * (1 if number > 1 or k < EARLY_OWN else 2)
            if number + 1 < len(stages):
                ready.append((arrival + HOP_TIME + (1.5 if stage is stage_plane else 0.0), k, number + 1))
        else:
            k, q = quarters.pop(0)
            with jax.named_scope(f"matmul_{k}"):
                matmul_quarter(k, q)
            clock += QUARTER_TIME * ROW_CHUNKS[k]
            if q == RING - 1:
                ready.append((clock + PAIR_TIME, k, 0))

    keep = keep_ref[pl.ds(ex, 1), :].astype(jnp.float32)
    rows = d_model // 8
    whole = fin[...] * (keep / scale)
    first, second = whole[0:rows, :], whole[whole.shape[0] - rows :, :]
    out_ref[...] = jnp.where(core == 0, first, second)

    taken(cnt_recv.at[0:7], csend.at[0])
    taken(cnt_recv.at[0:3], csend.at[1])
    taken(cnt_recv.at[0:3], csend.at[2])
    for k in range(max(chunks - 2, 0), chunks):
        pair_copy(k, 0, eblocks).wait_send()
    for k in range(chunks):
        taken(plane[k] if k in PLANE else umid[k].at[:, 0:3], ssem.at[k, 2])


def solution(mesh):
    devices = mesh.devices.size

    def local(tokens, router_logits, gate_grad, expert_index, keep_mask):
        tok_rows, d_model = tokens.shape
        experts = router_logits.shape[1]
        eblocks = experts // LANES
        chunks = len(ROW_CHUNKS)
        f32, bf16, i32 = jnp.float32, jnp.bfloat16, jnp.int32
        rmax = max(ROW_CHUNKS)
        vm = pltpu.VMEM

        def per_chunk(shape_of):
            return [vm(shape_of(r), f32) for r in ROW_CHUNKS]

        scratch = [
            vm((SLOTS, TB, experts), bf16),
            vm((tok_rows, LANES), i32),
            vm((tok_rows, LANES), f32),
            vm((tok_rows, LANES), f32),
            vm((tok_rows, experts), f32),
            [vm((RING, tok_rows, LANES), bf16)] * RING,
            [vm((RING, tok_rows, LANES), LOW)] * RING,
            vm((24 * sum(ROW_CHUNKS), tok_rows), bf16),
            vm((24 * sum(ROW_CHUNKS), tok_rows), LOW),
            vm((2, eblocks, 24 * rmax, LANES), f32),
            per_chunk(lambda r: (eblocks, 12 * r, LANES)),
            per_chunk(lambda r: (3, 4, 4, 4, r, LANES)),
            per_chunk(lambda r: (3, 2, 2, 4, r, LANES)),
            per_chunk(lambda r: (3, 2, 4, 4, r, LANES)),
            per_chunk(lambda r: (3, 4, 4, r, LANES)),
            per_chunk(lambda r: (3, 2, 2, r, LANES)),
            per_chunk(lambda r: (3, 2, 4, r, LANES)),
            per_chunk(lambda r: (3, 4, r, LANES)),
            per_chunk(lambda r: (3, 3, r, LANES)),
            [vm((3, RING * RING - 1, r if k in PLANE else 8, LANES), f32) for k, r in enumerate(ROW_CHUNKS)],
            vm((264, LANES), f32),
            vm((3, eblocks, LANES), i32),
            vm((13, eblocks, LANES), i32),
            vm((eblocks, LANES), f32),
            pltpu.SemaphoreType.DMA((SLOTS,)),
            pltpu.SemaphoreType.DMA((chunks,)),
            pltpu.SemaphoreType.DMA((3,)),
            pltpu.SemaphoreType.DMA((13,)),
            pltpu.SemaphoreType.DMA((chunks,)),
            pltpu.SemaphoreType.DMA((chunks,)),
            pltpu.SemaphoreType.DMA((chunks, 3)),
            pltpu.SemaphoreType.DMA((chunks, 3, 7)),
        ]
        return pl.pallas_call(
            functools.partial(kernel, tok_rows * devices),
            out_shape=jax.ShapeDtypeStruct((d_model // 8, LANES), f32),
            in_specs=[pl.BlockSpec(memory_space=pltpu.VMEM)] * 3 + [pl.BlockSpec(memory_space=pl.ANY)] * 2,
            out_specs=pl.BlockSpec(memory_space=pltpu.VMEM),
            scratch_shapes=scratch,
            compiler_params=pltpu.CompilerParams(collective_id=0, has_side_effects=True, vmem_limit_bytes=67043328),
        )(
            expert_index.reshape(tok_rows // LANES, LANES),
            gate_grad.reshape(tok_rows // LANES, LANES),
            keep_mask.reshape(eblocks, LANES),
            tokens.T,
            router_logits,
        ).T

    return jax.shard_map(
        local,
        mesh=mesh,
        in_specs=(P(("dp", "expert"), None), P(("dp", "expert"), None), P(("dp", "expert")), P(("dp", "expert"), None), P()),
        out_specs=P("expert", "dp"),
        check_vma=False,
    )
```

```python
import functools

import jax
import jax.numpy as jnp
from jax import lax
from jax.experimental import pallas as pl
from jax.experimental.pallas import tpu as pltpu
from jax.sharding import PartitionSpec as P

MESH = pl.DeviceIdType.MESH
RING = 4
LOW = jnp.float8_e5m2
PAIR_TIME, HOP_TIME, QUARTER_TIME = 1.1, 2.4, 0.046
PLANE = (6,)
EARLY_OWN = 6
LANES = 128
ROW_CHUNKS = (8, 16, 16, 16, 16, 8, 8)
TB = 128
SLOTS = 3


def kernel(total_tokens, idx_ref, gate_ref, keep_ref, tok_ref, logit_ref, out_ref,
           lbuf, icol, acol, drop, ptab, gmat, glow, xt, xlow, cbuf, drecv, sums, r1m, r1f, tmid, r2m, r2f, umid, r3, plane,
           fin, cnt, cnt_recv, aux_ref,
           lsem, xsem, csend, crecv, dsend, drsem, ssem, rsem):
    d_model, tok_rows = tok_ref.shape
    experts = logit_ref.shape[1]
    eblocks = experts // LANES
    blocks = tok_rows // TB
    chunks = len(ROW_CHUNKS)
    offsets = [sum(ROW_CHUNKS[:k]) for k in range(chunks)]

    dp = lax.axis_index("dp")
    ex = lax.axis_index("expert")
    zc, core = dp // 2, dp % 2
    yc, xc = ex // RING, ex % RING
    here = {"x": xc, "y": yc, "z": zc}

    def device(**moved):
        at = dict(here, **moved)
        return (2 * at["z"] + core, RING * at["y"] + at["x"])

    sibling = (2 * zc + 1 - core, ex)
    same_column = [((dp + step) % 8, ex) for step in range(1, 8)]

    def away(axis, step):
        return device(**{axis: (here[axis] + step) % RING})

    def load_logits(b, slot):
        return pltpu.make_async_copy(logit_ref.at[pl.ds(b * TB, TB), :], lbuf.at[slot], lsem.at[slot])

    for b in range(SLOTS):
        load_logits(b, b).start()

    barrier = pltpu.get_barrier_semaphore()
    peers = same_column + [away(axis, step) for axis in "xy" for step in (1, 2, 3)]
    for peer in peers:
        pl.semaphore_signal(barrier, inc=1, device_id=peer, device_id_type=MESH)

    idx = idx_ref[...]
    total = jnp.zeros((eblocks, LANES), jnp.float32)
    for b in range(blocks):
        row = idx[b : b + 1, :]
        high = (row // LANES == lax.broadcasted_iota(jnp.int32, (eblocks, LANES), 0)).astype(jnp.bfloat16)
        low = (row % LANES == lax.broadcasted_iota(jnp.int32, (LANES, LANES), 0)).astype(jnp.bfloat16)
        total = total + lax.dot_general(high, low, (((1,), (1,)), ((), ())), preferred_element_type=jnp.float32)
    cnt[0] = total.astype(jnp.int32)

    def count_copies(stage):
        targets = same_column if stage == 0 else [away("xy"[stage - 1], step) for step in (1, 2, 3)]
        first = (0, 7, 10)[stage]
        return [
            pltpu.make_async_remote_copy(cnt.at[stage], cnt_recv.at[first + n], csend.at[stage], crecv.at[first + n], device_id=target, device_id_type=MESH)
            for n, target in enumerate(targets)
        ]

    def count_arrive(stage):
        value = cnt[stage]
        for number, copy in enumerate(count_copies(stage)):
            copy.wait_recv()
            value = value + cnt_recv[(0, 7, 10)[stage] + number]
        return value

    def count_step(stage):
        cnt[stage + 1] = count_arrive(stage)
        for copy in count_copies(stage + 1):
            copy.start()

    idx_t = jnp.transpose(idx.astype(jnp.float32))
    gate_t = jnp.transpose(gate_ref[...])
    for b in range(blocks):
        icol[b * TB : (b + 1) * TB, :] = jnp.broadcast_to(idx_t[:, b : b + 1], (TB, LANES)).astype(jnp.int32)
        acol[b * TB : (b + 1) * TB, :] = jnp.broadcast_to(gate_t[:, b : b + 1], (TB, LANES))

    RS = 32

    def lane_of(j):
        return lax.broadcasted_iota(jnp.int32, (RS, LANES), 1) + j * LANES

    def stats_block(b):
        slot = b % SLOTS
        load_logits(b, slot).wait()

        def rows(r, carry):
            local = pl.ds(pl.multiple_of(r * RS, RS), RS)
            at = pl.ds(pl.multiple_of(b * TB + r * RS, RS), RS)
            peak = lbuf[slot, local, 0:LANES].astype(jnp.float32)
            for j in range(1, eblocks):
                peak = jnp.maximum(peak, lbuf[slot, local, j * LANES : (j + 1) * LANES].astype(jnp.float32))
            peak = jnp.max(peak, axis=1, keepdims=True)
            mass = jnp.zeros((RS, LANES), jnp.float32)
            top = jnp.zeros((RS, LANES), jnp.float32)
            chosen = icol[at, :]
            for j in range(eblocks):
                weight = jnp.exp(lbuf[slot, local, j * LANES : (j + 1) * LANES].astype(jnp.float32) - peak)
                ptab[at, j * LANES : (j + 1) * LANES] = weight
                mass = mass + weight
                top = top + jnp.where(chosen == lane_of(j), weight, 0.0)
            inverse = 1.0 / jnp.sum(mass, axis=1, keepdims=True)
            top_prob = jnp.sum(top, axis=1, keepdims=True) * inverse
            acol[at, :] = acol[at, :] * top_prob
            for j in range(eblocks):
                ptab[at, j * LANES : (j + 1) * LANES] = ptab[at, j * LANES : (j + 1) * LANES] * inverse
            return carry

        lax.fori_loop(0, TB // RS, rows, 0)

    def prep(b, carry):
        stats_block(b)

        @pl.when(b + SLOTS < blocks)
        def _():
            load_logits(b + SLOTS, b % SLOTS).start()

        return carry

    with jax.named_scope("prep_0"):
        lax.fori_loop(0, 1, prep, 0)
    with jax.named_scope("barrier"):
        pl.semaphore_wait(barrier, len(peers))
    for copy in count_copies(0):
        copy.start()

    for k in range(chunks):
        r = ROW_CHUNKS[k]
        for group in range(24):
            cc, zz, part = group // 12, (group // 3) % 4, group % 3
            src = (d_model // RING) * zz + 256 * cc + 88 * part + offsets[k]
            dst = 24 * offsets[k] + r * group
            pltpu.make_async_copy(tok_ref.at[pl.ds(src, r), :], xt.at[pl.ds(dst, r), :], xsem.at[k]).start()

    with jax.named_scope("prep_1"):
        lax.fori_loop(1, 5, prep, 0)
    with jax.named_scope("count_step_0"):
        count_step(0)
    with jax.named_scope("prep_2"):
        lax.fori_loop(5, 7, prep, 0)
    with jax.named_scope("count_step_1"):
        count_step(1)
    with jax.named_scope("prep_3"):
        lax.fori_loop(7, 8, prep, 0)
    def lower_rows(n, carry):
        at = pl.ds(pl.multiple_of(n * LR, LR), LR)
        xlow[at, :] = xt[at, :].astype(LOW)
        return carry

    LR = 96
    with jax.named_scope("lower"):
        for k in range(chunks):
            chunk_rows = xt.at[pl.ds(24 * offsets[k], 24 * ROW_CHUNKS[k]), :]
            pltpu.make_async_copy(chunk_rows, chunk_rows, xsem.at[k]).wait()
        lax.fori_loop(0, 24 * sum(ROW_CHUNKS) // LR, lower_rows, 0)

    with jax.named_scope("count_last"):
        raw = count_arrive(2).astype(jnp.float32) * (experts / total_tokens)
        scale = 4194304.0 / (jnp.max(jnp.max(raw, axis=1, keepdims=True), axis=0, keepdims=True) + 6.0)
        aux_ref[...] = raw * scale

    def spread_rows(r, carry):
        at = pl.ds(pl.multiple_of(r * RS, RS), RS)
        acc = ptab[at, 0:LANES] * aux_ref[0:1, :]
        for j in range(1, eblocks):
            acc = acc + ptab[at, j * LANES : (j + 1) * LANES] * aux_ref[j : j + 1, :]
        gain = acol[at, :] * scale
        acol[at, :] = gain
        drop[at, :] = jnp.sum(acc, axis=1, keepdims=True) + gain
        return carry

    with jax.named_scope("spread"):
        lax.fori_loop(0, tok_rows // RS, spread_rows, 0, unroll=8)

    def grad_piece(q, row):
        gain = acol[row : row + RS, :]
        less = drop[row : row + RS, :]
        chosen = icol[row : row + RS, :]
        for j in range(RING * q, RING * q + RING):
            value = ptab[row : row + RS, j * LANES : (j + 1) * LANES] * (aux_ref[j : j + 1, :] - less)
            value = jnp.where(chosen == lane_of(j), value + gain, value)
            big = value.astype(jnp.bfloat16)
            gmat[q][j - RING * q, row : row + RS, :] = big
            glow[q][j - RING * q, row : row + RS, :] = (value - big.astype(jnp.float32)).astype(LOW)

    def pair_copy(k, first, count):
        rows = 12 * ROW_CHUNKS[k]
        src = cbuf.at[k % 2, pl.ds(first, count), pl.ds(pl.multiple_of((1 - core) * rows, 8), rows), :]
        return pltpu.make_async_remote_copy(
            src, drecv[k].at[pl.ds(first, count)], dsend.at[k], drsem.at[k], device_id=sibling, device_id_type=MESH)

    NT, KT = 256, 256

    def matmul_quarter(k, q, beside=()):
        rows = 24 * ROW_CHUNKS[k]
        base = 24 * offsets[k]
        if q == 0:
            if k >= 2:
                pair_copy(k - 2, 0, eblocks).wait_send()
        count = experts // RING // NT * 2 * (tok_rows // KT)
        beside = list(beside)
        each = -(-len(beside) // count)
        for n in range(experts // RING // NT):
            value = None
            for half in range(2):
                for kt in range(tok_rows // KT):
                    left, right = ((xt, gmat), (xlow, glow))[half]
                    right = [right[q][n * (NT // LANES) + j, kt * KT : (kt + 1) * KT, :] for j in range(NT // LANES)]
                    part = jnp.dot(
                        left[base : base + rows, kt * KT : (kt + 1) * KT], jnp.concatenate(right, axis=1), preferred_element_type=jnp.float32)
                    value = part if value is None else value + part
                    for piece in beside[:each]:
                        piece()
                    beside = beside[each:]
            for j in range(NT // LANES):
                cbuf[k % 2, RING * q + n * (NT // LANES) + j, 0:rows, :] = value[:, j * LANES : (j + 1) * LANES]
        pair_copy(k, RING * q, RING).start()

    orders = ("xyz", "yzx", "zxy")

    def pos(p, stage):
        return here[orders[p][stage]]

    def around(k, p, stage, numbers):
        axis, i = orders[p][stage], pos(p, stage)
        up, down, far = (i + 1) % RING, (i + 3) % RING, (i + 2) % RING
        right, left = away(axis, 1), away(axis, 3)
        s = (sums, tmid)[stage][k].at[p]
        m = (r1m, r2m)[stage][k].at[p]
        f = (r1f, r2f)[stage][k].at[p]
        table = (
            (s.at[far, 0:2], m.at[0], 0, right),
            (s.at[far, 2:4], m.at[1], 1, left),
            (s.at[up, 2:4], f.at[0, 2:4], 2, right),
            (s.at[down, 0:2], f.at[1, 0:2], 2, left),
            (s.at[up, 0:2], f.at[0, 0:2], 2, right),
            (s.at[down, 2:4], f.at[1, 2:4], 2, left),
            (s.at[up], f.at[0], 2, right),
            (s.at[down], f.at[1], 2, left),
        )
        copies = []
        for n in numbers:
            src, dst, sem, peer = table[n]
            copies.append(pltpu.make_async_remote_copy(src, dst, ssem.at[k, stage], rsem.at[k, p, 3 * stage + sem], device_id=peer, device_id_type=MESH))
        return copies

    def last_ring(k, p):
        axis, i = orders[p][2], pos(p, 2)
        return [
            pltpu.make_async_remote_copy(
                umid[k].at[p, (i + step) % RING], r3[k].at[p, step - 1], ssem.at[k, 2], rsem.at[k, p, 6], device_id=away(axis, step), device_id_type=MESH)
            for step in (1, 2, 3)
        ]

    def taken(ref, sem):
        pltpu.make_async_copy(ref, ref, sem).wait()

    def merge(k, p, stage):
        i = pos(p, stage)
        up, down = (i + 1) % RING, (i + 3) % RING
        s, m = (sums, tmid)[stage][k], (r1m, r2m)[stage][k]
        early = stage == 0 and k < EARLY_OWN
        first, second, third, fourth = around(k, p, stage, (0, 1, 4, 5) if early else (0, 1, 6, 7))
        first.wait_recv()
        s[p, up, 0:2] = s[p, up, 0:2] + m[p, 0]
        third.start()
        second.wait_recv()
        s[p, down, 2:4] = s[p, down, 2:4] + m[p, 1]
        fourth.start()

    def stage_a(k):
        pair_copy(k, 0, eblocks).wait_recv()
        r = ROW_CHUNKS[k]

        def block(e, carry):
            ye, xe = e // RING, e % RING
            for zz in range(RING):
                for p in range(3):
                    row = (zz * 3 + p) * r
                    mine = pl.ds(pl.multiple_of(core * (12 * r) + row, 8), r)
                    value = cbuf[k % 2, e, mine, :] + drecv[k][e, row : row + r, :]
                    at = {"x": xe, "y": ye, "z": zz}
                    sums[k][p, at[orders[p][0]], at[orders[p][1]], at[orders[p][2]]] = value
            return carry

        lax.fori_loop(0, eblocks, block, 0)
        for n in range(4 if k < EARLY_OWN else 2):
            for p in range(3):
                around(k, p, 0, (n,))[0].start()

    def stage_b(k):
        for p in range(3):
            merge(k, p, 0)

    def stage_c(k):
        for p in range(3):
            taken(r1f[k].at[p], rsem.at[k, p, 2])
            tmid[k][p] = sums[k][p, pos(p, 0)] + r1f[k][p, 0] + r1f[k][p, 1]
            for copy in around(k, p, 1, (0, 1)):
                copy.start()

    def stage_d(k):
        for p in range(3):
            merge(k, p, 1)

    def stage_e(k):
        for p in range(3):
            taken(r2f[k].at[p], rsem.at[k, p, 5])
            umid[k][p] = tmid[k][p, pos(p, 1)] + r2f[k][p, 0] + r2f[k][p, 1]
            for copy in last_ring(k, p):
                copy.start()
        taken(sums[k].at[:, 0:3], ssem.at[k, 0])

    def stage_f(k):
        r = ROW_CHUNKS[k]
        for p in range(3):
            taken(r3[k].at[p], rsem.at[k, p, 6])
            row = 88 * p + offsets[k]
            fin[row : row + r, :] = umid[k][p, pos(p, 2)] + r3[k][p, 0] + r3[k][p, 1] + r3[k][p, 2]
        taken(tmid[k].at[:, 0:3], ssem.at[k, 1])

    def plane_ring(k, p):
        (one, i), (two, j) = (orders[p][1], pos(p, 1)), (orders[p][2], pos(p, 2))
        copies = []
        for n in range(1, RING * RING):
            b, c = (i + n // RING) % RING, (j + n % RING) % RING
            copies.append(pltpu.make_async_remote_copy(
                tmid[k].at[p, b, c], plane[k].at[p, n - 1], ssem.at[k, 2], rsem.at[k, p, 6], device_id=device(**{one: b, two: c}), device_id_type=MESH))
        return copies

    def stage_plane(k):
        for p in range(3):
            taken(r1f[k].at[p], rsem.at[k, p, 2])
            tmid[k][p] = sums[k][p, pos(p, 0)] + r1f[k][p, 0] + r1f[k][p, 1]
            for copy in plane_ring(k, p):
                copy.start()
        taken(sums[k].at[:, 0:3], ssem.at[k, 0])

    def stage_g(k):
        r = ROW_CHUNKS[k]
        for p in range(3):
            taken(plane[k].at[p], rsem.at[k, p, 6])
            row = 88 * p + offsets[k]
            value = tmid[k][p, pos(p, 1), pos(p, 2)]
            for n in range(RING * RING - 1):
                value = value + plane[k][p, n]
            fin[row : row + r, :] = value

    def grad_pieces(q):
        return [functools.partial(grad_piece, q, row) for row in range(0, tok_rows, RS)]

    with jax.named_scope("first_chunk"):
        for piece in grad_pieces(0):
            piece()
        for q in range(RING):
            matmul_quarter(0, q, grad_pieces(q + 1) if q + 1 < RING else ())

    ring_stages = ((stage_a, 0.0), (stage_b, 0.088), (stage_c, 0.022), (stage_d, 0.044), (stage_e, 0.033), (stage_f, 0.0))
    plane_stages = ((stage_a, 0.0), (stage_b, 0.088), (stage_plane, 0.175), (stage_g, 0.0))
    quarters = [(k, q) for k in range(1, chunks) for q in range(RING)]
    ready = [(PAIR_TIME, 0, 0)]
    clock, links = 0.0, 0.0
    while quarters or ready:
        ready.sort()
        if ready and (ready[0][0] <= clock or not quarters):
            when, k, number = ready.pop(0)
            stages = plane_stages if k in PLANE else ring_stages
            stage, wire = stages[number]
            r = ROW_CHUNKS[k]
            clock = max(clock, when) + (0.04 if number else 0.025 * r)
            with jax.named_scope(f"{stage.__name__}_{k}"):
                stage(k)
            if number == 0:
                arrival = max(clock, links) + 0.088 * r
                links = arrival + (0.088 * r if k < EARLY_OWN else 0.0)
            else:
                arrival = links = max(clock, links) + wire * r * (1 if number > 1 or k < EARLY_OWN else 2)
            if number + 1 < len(stages):
                ready.append((arrival + HOP_TIME + (1.5 if stage is stage_plane else 0.0), k, number + 1))
        else:
            k, q = quarters.pop(0)
            with jax.named_scope(f"matmul_{k}"):
                matmul_quarter(k, q)
            clock += QUARTER_TIME * ROW_CHUNKS[k]
            if q == RING - 1:
                ready.append((clock + PAIR_TIME, k, 0))

    keep = keep_ref[pl.ds(ex, 1), :].astype(jnp.float32)
    rows = d_model // 8
    whole = fin[...] * (keep / scale)
    first, second = whole[0:rows, :], whole[whole.shape[0] - rows :, :]
    out_ref[...] = jnp.where(core == 0, first, second)

    taken(cnt_recv.at[0:7], csend.at[0])
    taken(cnt_recv.at[0:3], csend.at[1])
    taken(cnt_recv.at[0:3], csend.at[2])
    for k in range(max(chunks - 2, 0), chunks):
        pair_copy(k, 0, eblocks).wait_send()
    for k in range(chunks):
        taken(plane[k] if k in PLANE else umid[k].at[:, 0:3], ssem.at[k, 2])


def solution(mesh):
    devices = mesh.devices.size

    def local(tokens, router_logits, gate_grad, expert_index, keep_mask):
        tok_rows, d_model = tokens.shape
        experts = router_logits.shape[1]
        eblocks = experts // LANES
        chunks = len(ROW_CHUNKS)
        f32, bf16, i32 = jnp.float32, jnp.bfloat16, jnp.int32
        rmax = max(ROW_CHUNKS)
        vm = pltpu.VMEM

        def per_chunk(shape_of):
            return [vm(shape_of(r), f32) for r in ROW_CHUNKS]

        scratch = [
            vm((SLOTS, TB, experts), bf16),
            vm((tok_rows, LANES), i32),
            vm((tok_rows, LANES), f32),
            vm((tok_rows, LANES), f32),
            vm((tok_rows, experts), f32),
            [vm((RING, tok_rows, LANES), bf16)] * RING,
            [vm((RING, tok_rows, LANES), LOW)] * RING,
            vm((24 * sum(ROW_CHUNKS), tok_rows), bf16),
            vm((24 * sum(ROW_CHUNKS), tok_rows), LOW),
            vm((2, eblocks, 24 * rmax, LANES), f32),
            per_chunk(lambda r: (eblocks, 12 * r, LANES)),
            per_chunk(lambda r: (3, 4, 4, 4, r, LANES)),
            per_chunk(lambda r: (3, 2, 2, 4, r, LANES)),
            per_chunk(lambda r: (3, 2, 4, 4, r, LANES)),
            per_chunk(lambda r: (3, 4, 4, r, LANES)),
            per_chunk(lambda r: (3, 2, 2, r, LANES)),
            per_chunk(lambda r: (3, 2, 4, r, LANES)),
            per_chunk(lambda r: (3, 4, r, LANES)),
            per_chunk(lambda r: (3, 3, r, LANES)),
            [vm((3, RING * RING - 1, r if k in PLANE else 8, LANES), f32) for k, r in enumerate(ROW_CHUNKS)],
            vm((264, LANES), f32),
            vm((3, eblocks, LANES), i32),
            vm((13, eblocks, LANES), i32),
            vm((eblocks, LANES), f32),
            pltpu.SemaphoreType.DMA((SLOTS,)),
            pltpu.SemaphoreType.DMA((chunks,)),
            pltpu.SemaphoreType.DMA((3,)),
            pltpu.SemaphoreType.DMA((13,)),
            pltpu.SemaphoreType.DMA((chunks,)),
            pltpu.SemaphoreType.DMA((chunks,)),
            pltpu.SemaphoreType.DMA((chunks, 3)),
            pltpu.SemaphoreType.DMA((chunks, 3, 7)),
        ]
        return pl.pallas_call(
            functools.partial(kernel, tok_rows * devices),
            out_shape=jax.ShapeDtypeStruct((d_model // 8, LANES), f32),
            in_specs=[pl.BlockSpec(memory_space=pltpu.VMEM)] * 3 + [pl.BlockSpec(memory_space=pl.ANY)] * 2,
            out_specs=pl.BlockSpec(memory_space=pltpu.VMEM),
            scratch_shapes=scratch,
            compiler_params=pltpu.CompilerParams(collective_id=0, has_side_effects=True, vmem_limit_bytes=67043328),
        )(
            expert_index.reshape(tok_rows // LANES, LANES),
            gate_grad.reshape(tok_rows // LANES, LANES),
            keep_mask.reshape(eblocks, LANES),
            tokens.T,
            router_logits,
        ).T

    return jax.shard_map(
        local,
        mesh=mesh,
        in_specs=(P(("dp", "expert"), None), P(("dp", "expert"), None), P(("dp", "expert")), P(("dp", "expert"), None), P()),
        out_specs=P("expert", "dp"),
        check_vma=False,
    )
```
